8 devices in a mesh: dp: 1 (over z), ep: 8 (over x, y, core).
Axes of the slice: x: 2, y: 2, z: 1, core: 2. Of those that a mesh axis runs over, the one named last changes fastest.
Arguments:
- x: bfloat16 [1, 8, 256, 7168], P('dp', 'ep')
- expert: int32 [1, 8, 256, 8], P('dp', 'ep')
- slot: int32 [1, 8, 256, 8], P('dp', 'ep')
- gate: float32 [1, 8, 256, 8], P('dp', 'ep')
- w_gate: bfloat16 [32, 7168, 2048], P('ep')
- w_up: bfloat16 [32, 7168, 2048], P('ep')
- w_down: bfloat16 [32, 2048, 7168], P('ep')
- s_gate: bfloat16 [7168, 2048], replicated
- s_up: bfloat16 [7168, 2048], replicated
- s_down: bfloat16 [2048, 7168], replicated
Outputs:
- y: bfloat16 [1, 8, 256, 7168], P('dp', 'ep')
All inputs are finite; a program needn't handle non-finite values.
Results may differ from the reference program's by a relative error of at most 0.009.
Values are sent between devices in bfloat16 or wider.
A program may use at most 2 GiB of HBM per device.

```python
import jax
import jax.numpy as jnp

MEMBERS = 8
TOKENS = 256
D = 7168
FF = 2048
TOP = 8
EXPERTS = 32
SHARED_FF = 2048
SLOTS = 5 * TOKENS * TOP // (4 * EXPERTS)


def setup_inputs(seed: int = 0, part: int = 0) -> dict:
    own, k1, k2, k3, k4, k5, k6 = jax.random.split(jax.random.key(seed), 7)
    kx, ke, kl, kg = jax.random.split(jax.random.fold_in(own, part), 4)
    devices = (1, MEMBERS)
    place = jax.random.permutation(kl, jnp.arange(EXPERTS, dtype=jnp.uint32))
    slow = ((EXPERTS + (9 * place) % EXPERTS) << ((9 * place) // EXPERTS)) // EXPERTS
    wait = (jax.random.bits(ke, (*devices, TOKENS, EXPERTS), jnp.uint32) >> 10) * slow
    expert = jnp.argsort(wait, axis=-1)[..., :TOP].astype(jnp.int32)
    chosen = jax.nn.one_hot(expert, EXPERTS, dtype=jnp.int32)
    in_line = jnp.cumsum(chosen.reshape(*devices, TOKENS * TOP, EXPERTS), axis=2) - 1
    slot = jnp.sum(in_line.reshape(chosen.shape) * chosen, axis=-1)

    def one(key, rows, columns):
        return (jax.random.normal(key, (rows, columns), jnp.float32) * rows**-0.5).astype(jnp.bfloat16)

    def weights(key, rows, columns):
        return jax.lax.map(lambda k: one(k, rows, columns), jax.random.split(key, EXPERTS))

    return {
        "x": jax.random.normal(kx, (*devices, TOKENS, D), jnp.float32).astype(jnp.bfloat16),
        "expert": expert,
        "slot": slot,
        "gate": jax.nn.softmax(jax.random.normal(kg, expert.shape, jnp.float32)),
        "w_gate": weights(k1, D, FF),
        "w_up": weights(k2, D, FF),
        "w_down": weights(k3, FF, D),
        "s_gate": one(k4, D, SHARED_FF),
        "s_up": one(k5, D, SHARED_FF),
        "s_down": one(k6, SHARED_FF, D),
    }


def einsum(form, a, b):
    return jnp.einsum(form, a.astype(jnp.float32), b.astype(jnp.float32))


def for_all(x, s_gate, s_up, s_down):
    h = jax.nn.silu(einsum("...d,df->...f", x, s_gate)) * einsum("...d,df->...f", x, s_up)
    return einsum("...f,fd->...d", h.astype(jnp.bfloat16), s_down)


def reference(x, expert, slot, gate, w_gate, w_up, w_down, s_gate, s_up, s_down):
    to_expert = jax.nn.one_hot(expert, EXPERTS, dtype=jnp.bfloat16)
    to_slot = jax.nn.one_hot(slot, SLOTS, dtype=jnp.bfloat16)
    weighted = to_expert * gate[..., None].astype(jnp.bfloat16)
    dispatch = einsum("abtke,abtkc->abtec", to_expert, to_slot).astype(jnp.bfloat16)
    combine = einsum("abtke,abtkc->abtec", weighted, to_slot).astype(jnp.bfloat16)
    z = einsum("abtec,abtd->aebcd", dispatch, x).astype(jnp.bfloat16)
    h = jax.nn.silu(einsum("aebcd,edf->aebcf", z, w_gate))
    h = (h * einsum("aebcd,edf->aebcf", z, w_up)).astype(jnp.bfloat16)
    out = einsum("aebcf,efd->aebcd", h, w_down).astype(jnp.bfloat16)
    y = einsum("abtec,aebcd->abtd", combine, out)
    return (y + for_all(x, s_gate, s_up, s_down)).astype(jnp.bfloat16)
```

```python
import jax
import jax.numpy as jnp
from jax import lax
from jax.experimental import pallas as pl
from jax.experimental.pallas import tpu as pltpu
from jax.sharding import PartitionSpec as P

MESH = pl.DeviceIdType.MESH
F32, BF16 = jnp.float32, jnp.bfloat16
N = 8
T = 256
D = 7168
FF = 2048
TOP = 8
E = 4
CAP = 80
SEG = E * CAP
ROWS = N * SEG
PER = N * CAP
KB = 512
NK = D // KB
NB = 512
CB = 512
HB = CB // 2
NC = D // CB
WRING = 3
DRING = 4


def around(me):
    i, j, c = me // 4, (me // 2) % 2, me % 2
    at = lambda i, j, c: i * 4 + j * 2 + c
    return at(i, j, 1 - c), at(1 - i, j, c), at(i, 1 - j, c), at(1 - i, 1 - j, c)


def greet(devices):
    barrier = pltpu.get_barrier_semaphore()
    for d in devices:
        pl.semaphore_signal(barrier, inc=1, device_id={"ep": d}, device_id_type=MESH)
    pl.semaphore_wait(barrier, len(devices))


def remote(src, dst, send, recv, to):
    return pltpu.make_async_remote_copy(
        src_ref=src, dst_ref=dst, send_sem=send, recv_sem=recv, device_id={"ep": to}, device_id_type=MESH
    )


def dot(a, b):
    return jnp.dot(a, b, preferred_element_type=F32)


def up_kernel(
    x, table, wg, wu, sg, su, xg, tables, h, sh,
    acc_g, acc_u, z, xv, wv, pick, tv,
    w_sem, xv_sem, out_sem, t_send, t_recv, o_send, o_recv, f_send, f_recv, c_send, c_recv,
):
    me = lax.axis_index("ep")
    cn, xn, yn, dg = around(me)
    others = [lax.rem(me + d, N) for d in range(1, N)]

    def weights(s, run):
        slot = lax.rem(s, WRING)

        def two(a, b):
            for half, ref in ((0, a), (1, b)):
                run(pltpu.make_async_copy(ref, wv.at[slot, half], w_sem.at[slot, half]))

        @pl.when(s < NK)
        def _():
            rows = pl.ds(pl.multiple_of(s * KB, KB), KB)
            two(sg.at[rows], su.at[rows])

        @pl.when(jnp.logical_and(s >= NK, s < NK + NK * E))
        def _():
            k, e = (s - NK) // E, (s - NK) % E
            rows = pl.ds(pl.multiple_of(k * KB, KB), KB)
            two(wg.at[e, rows], wu.at[e, rows])

    for s in range(WRING - 1):
        weights(s, lambda c: c.start())

    def cols(k):
        return pl.ds(pl.multiple_of(k * KB, KB), KB)

    for k in range(NK):
        pltpu.make_async_copy(x.at[:, cols(k)], xv.at[k // N, k % N], xv_sem.at[k // N, k % N]).start()

    greet(others)
    for i, d in enumerate(others):
        remote(table, tv.at[me], t_send.at[i], t_recv.at[N - 2 - i], d).start()
    keep = pltpu.make_async_copy(table, tv.at[me], out_sem.at[0])
    keep.start()

    def own(k, run):
        for i, d in enumerate((xn, yn, cn)):
            run(remote(x.at[:, cols(k)], xg.at[me, :, cols(k)], o_send.at[i, k], o_recv.at[i, k], d))

    def forward(k, run):
        p = lax.rem(k, 2)
        src, to = xn * (1 - p) + yn * p, yn * (1 - p) + xn * p
        part = xg.at[src, :, cols(k)]
        run(remote(part, part, f_send.at[k], f_recv.at[k], to))

    def across(i, src, k, run):
        part = xg.at[src, :, cols(k)]
        run(remote(part, part, c_send.at[i, k], c_recv.at[i, k], cn))

    start, wait_send, wait_recv = (lambda c: c.start()), (lambda c: c.wait_send()), (lambda c: c.wait_recv())

    def arrived(i, src, k):
        part = xg.at[src, :, cols(k)]
        remote(part, part, o_send.at[i, k], o_recv.at[i, k], xn).wait_recv()

    def stage_own(k):
        @pl.when(k < NK)
        def _():
            own(k, start)

    def stage_forward(k):
        @pl.when(k < NK)
        def _():
            arrived(0, xn, k)
            arrived(1, yn, k)
            forward(k, start)
            across(0, xn, k, start)
            across(1, yn, k, start)

    def stage_across(k):
        @pl.when(k < NK)
        def _():
            part = xg.at[dg, :, cols(k)]
            remote(part, part, f_send.at[k], f_recv.at[k], xn).wait_recv()
            across(2, dg, k, start)

    def tokens(k, run):
        slot = lax.rem(k, 2)
        for d in range(1, N):
            b = lax.rem(me + d, N)
            run(pltpu.make_async_copy(xg.at[b, :, cols(k)], xv.at[slot, b], xv_sem.at[slot, b]))
        run(pltpu.make_async_copy(x.at[:, cols(k)], xv.at[slot, me], xv_sem.at[slot, me]))

    def stage_tokens(k):
        @pl.when(k < NK)
        def _():
            arrived(2, cn, k)
            for i in range(3):
                part = xg.at[cn, :, cols(k)]
                remote(part, part, c_send.at[i, k], c_recv.at[i, k], cn).wait_recv()
            tokens(k, start)

    stage_own(0)
    stage_own(1)

    def block(n):
        return pl.ds(pl.multiple_of(n * NB, NB), NB)

    def shared(s, first):
        weights(s + WRING - 1, lambda c: c.start())
        weights(s, lambda c: c.wait())
        a = (s // N, lax.rem(s, N))
        pltpu.make_async_copy(x.at[:, cols(s)], xv.at[a], xv_sem.at[a]).wait()
        slot = lax.rem(s, WRING)

        for n in range(FF // NB):
            for half, acc in ((0, acc_g), (1, acc_u)):
                b = slice(n * NB, (n + 1) * NB)
                v = dot(xv[a], wv[slot, half, :, b])
                acc[:T, b] = v if first else acc[:T, b] + v

    shared(0, True)

    def shared_body(s, c):
        @pl.when(s == NK // 2)
        def _():
            stage_forward(0)
            stage_own(2)

        shared(s, False)
        return c

    lax.fori_loop(1, NK, shared_body, 0)

    def shared_out(n, run):
        run(pltpu.make_async_copy(z.at[n * T:(n + 1) * T], sh.at[:, n * NB:(n + 1) * NB], out_sem.at[n]))

    keep.wait()
    for n in range(FF // NB):
        b = slice(n * NB, (n + 1) * NB)
        z[n * T:(n + 1) * T] = (jax.nn.silu(acc_g[:T, b]) * acc_u[:T, b]).astype(BF16)

    for i in range(N - 1):
        b = lax.rem(me + 1 + i, N)
        remote(table, tv.at[b], t_send.at[i], t_recv.at[i], b).wait_recv()
    for n in range(FF // NB):
        shared_out(n, lambda c: c.start())
    row = (lax.broadcasted_iota(jnp.int32, (SEG, T), 0) + me * SEG).astype(F32)

    def picks(b, c):
        hit = jnp.zeros((SEG, T), F32)
        for j in range(TOP):
            hit = hit + jnp.where(tv[b, j:j + 1, :] == row, 1.0, 0.0)
        pick[b] = hit.astype(BF16)
        return c

    lax.fori_loop(0, N, picks, 0)
    keep_tables = pltpu.make_async_copy(tv, tables, xv_sem.at[2, 0])
    keep_tables.start()
    for n in range(FF // NB):
        shared_out(n, lambda c: c.wait())

    stage_forward(1)
    stage_own(3)
    stage_across(0)
    stage_tokens(0)

    def gather(k):
        slot = lax.rem(k, 2)
        tokens(k, lambda c: c.wait())

        for b in range(N):
            v = dot(pick[b], xv[slot, b]).astype(BF16)
            for e in range(E):
                z[e * PER + b * CAP:e * PER + (b + 1) * CAP] = v[e * CAP:(e + 1) * CAP]

    def expert(k, e, first):
        s = NK + k * E + e
        weights(s + WRING - 1, lambda c: c.start())
        weights(s, lambda c: c.wait())
        slot = lax.rem(s, WRING)
        rows = pl.ds(pl.multiple_of(e * PER, PER), PER)

        for n in range(FF // NB):
            for half, acc in ((0, acc_g), (1, acc_u)):
                b = slice(n * NB, (n + 1) * NB)
                v = dot(z[rows], wv[slot, half, :, b])
                acc[rows, b] = v if first else acc[rows, b] + v

    def chunk(k, first):
        gather(k)

        def body(e, c):
            expert(k, e, first)

            @pl.when(e == 0)
            def _():
                stage_forward(k + 2)
                stage_own(k + 4)

            @pl.when(e == 1)
            def _():
                stage_across(k + 1)

            @pl.when(e == 2)
            def _():
                stage_tokens(k + 1)

            return c

        lax.fori_loop(0, E, body, 0)

    chunk(0, True)

    def chunks(k, c):
        chunk(k, False)
        return c

    lax.fori_loop(1, NK, chunks, 0)

    def store(n, e, run):
        rows = pl.ds(pl.multiple_of(e * PER, PER), PER)
        run(pltpu.make_async_copy(z.at[rows], h.at[rows, block(n)], out_sem.at[e]))

    def finish(i, c):
        n, e = i // E, lax.rem(i, E)
        rows = pl.ds(pl.multiple_of(e * PER, PER), PER)

        @pl.when(n > 0)
        def _():
            store(n - 1, e, lambda c: c.wait())

        z[rows] = (jax.nn.silu(acc_g[rows, block(n)]) * acc_u[rows, block(n)]).astype(BF16)
        store(n, e, lambda c: c.start())
        return c

    lax.fori_loop(0, FF // NB * E, finish, 0)
    for e in range(E):
        store(FF // NB - 1, e, lambda c: c.wait())
    keep_tables.wait()
    for i, d in enumerate(others):
        remote(table, tv.at[me], t_send.at[i], t_recv.at[i], d).wait_send()

    def drain(k, c):
        own(k, wait_send)
        forward(k, wait_send)
        for i, src in enumerate((xn, yn, dg)):
            across(i, src, k, wait_send)
        return c

    lax.fori_loop(0, NK, drain, 0)


def down_kernel(
    h, tables, wd, sh, sd, y,
    hv, wv, sv, shv, tv, comb, out, d_out, d_in, p_out, p_in, q_out, q_in, yv,
    h_sem, w_sem, s_sem, m_sem, y_sem, d_send, d_recv, p_send, p_recv, q_send, q_recv,
):
    me = lax.axis_index("ep")
    cn, xn, yn, dg = around(me)

    def cols(n):
        return pl.ds(pl.multiple_of(n * CB, CB), CB)

    def weights(s, run):
        @pl.when(s < NC * E)
        def _():
            slot = lax.rem(s, DRING)
            run(pltpu.make_async_copy(wd.at[s % E, :, cols(s // E)], wv.at[slot], w_sem.at[slot]))

    def shared(n, run):
        slot = lax.rem(n, 2)
        run(pltpu.make_async_copy(sd.at[:, cols(n)], sv.at[slot], s_sem.at[slot]))

    def activations(e, run):
        rows = pl.ds(pl.multiple_of(e * PER, PER), PER)
        run(pltpu.make_async_copy(h.at[rows], hv.at[rows], h_sem.at[e]))

    start, wait = (lambda c: c.start()), (lambda c: c.wait())
    load_tables = pltpu.make_async_copy(tables, tv, m_sem.at[0])
    load_tables.start()
    load_sh = pltpu.make_async_copy(sh, shv, m_sem.at[1])
    for e in range(E):
        activations(e, start)
        if e < DRING - 1:
            weights(e, start)
    load_sh.start()
    greet((cn, xn, yn))

    load_tables.wait()
    wide = -(-SEG // 128) * 128
    row = (lax.broadcasted_iota(jnp.int32, (wide, T), 0) + me * SEG).astype(F32)
    inside = lax.broadcasted_iota(jnp.int32, (wide, T), 0) < SEG

    def combines(b, c):
        v = jnp.zeros((wide, T), F32)
        for j in range(TOP):
            v = v + jnp.where(tv[b, j:j + 1, :] == row, tv[b, TOP + j:TOP + j + 1, :], 0.0)
        comb[b] = jnp.where(inside, v, 0.0).T.astype(BF16)
        return c

    lax.fori_loop(0, N, combines, 0)
    load_sh.wait()

    def product(i):
        slot = lax.rem(i, 4)

        def body(e, c):
            s = i * E + e
            weights(s + DRING - 1, start)
            weights(s, wait)

            @pl.when(i == 0)
            def _():
                activations(e, wait)

            rows = pl.ds(pl.multiple_of(e * PER, PER), PER)
            v = dot(hv[rows], wv[lax.rem(s, DRING)]).astype(BF16)
            for b in range(N):
                out[slot, b, pl.ds(pl.multiple_of(e * CAP, 16), CAP)] = v[b * CAP:(b + 1) * CAP]
            return c

        lax.fori_loop(0, E, body, 0)

    def summed(b, n, lanes):
        return dot(comb[b][:, :SEG], out[lax.rem(n, 4), b, :, lanes])

    both, left, right = slice(0, CB), slice(0, HB), slice(HB, CB)

    def to_partner(n, run):
        slot = lax.rem(n, 2)
        run(remote(d_out.at[slot], d_in.at[lax.rem(n, 5)], d_send.at[slot], d_recv.at[n], cn))

    def first_hop(n, run):
        slot = lax.rem(n, 2)
        for i, d in enumerate((xn, yn)):
            run(remote(p_out.at[slot, i], p_in.at[n, i], p_send.at[slot, i], p_recv.at[n, i], d))

    def second_hop(n, run):
        slot = lax.rem(n, 2)
        for i, d in enumerate((yn, xn)):
            run(remote(q_out.at[slot, i], q_in.at[n, i], q_send.at[slot, i], q_recv.at[n, i], d))

    wait_send, wait_recv = (lambda c: c.wait_send()), (lambda c: c.wait_recv())

    def for_partner(n):
        cx, cy, cd = around(cn)[1:]
        slot = lax.rem(n, 2)

        @pl.when(n >= 2)
        def _():
            to_partner(n - 2, wait_send)

        for i, b in enumerate((cn, cx, cy, cd)):
            d_out[slot, i] = summed(b, n, both).astype(BF16)

    def for_first(n):
        slot, held = lax.rem(n, 2), lax.rem(n, 5)

        @pl.when(n >= 2)
        def _():
            first_hop(n - 2, wait_send)

        to_partner(n, wait_recv)
        v = (summed(dg, n, both) + d_in[held, 3].astype(F32)).astype(BF16)
        p_out[slot, 0, 1] = v[:, :HB]
        p_out[slot, 1, 1] = v[:, HB:]
        for i, (b, at, lanes) in enumerate(((xn, 1, left), (yn, 2, right))):
            p_out[slot, i, 0] = (summed(b, n, lanes) + d_in[held, at, :, lanes].astype(F32)).astype(BF16)

    def for_second(n):
        slot, held = lax.rem(n, 2), lax.rem(n, 5)

        @pl.when(n >= 2)
        def _():
            second_hop(n - 2, wait_send)

        first_hop(n, wait_recv)
        for i, (b, at, lanes) in enumerate(((yn, 2, left), (xn, 1, right))):
            v = summed(b, n, lanes) + d_in[held, at, :, lanes].astype(F32) + p_in[n, i, 1].astype(F32)
            q_out[slot, i] = v.astype(BF16)

    def result(n, run):
        slot = lax.rem(n, 2)
        run(pltpu.make_async_copy(yv.at[slot], y.at[:, cols(n)], y_sem.at[slot]))

    def for_own(n):
        slot, held = lax.rem(n, 2), lax.rem(n, 5)

        @pl.when(n >= 2)
        def _():
            result(n - 2, wait)

        shared(n, wait)
        v = dot(shv[...], sv[lax.rem(n, 2)])
        v = v + summed(me, n, both) + d_in[held, 0].astype(F32)
        second_hop(n, wait_recv)
        for i, lanes in enumerate((left, right)):
            w = v[:, lanes] + p_in[n, i, 0].astype(F32) + q_in[n, i].astype(F32)
            yv[slot, :, lanes] = w.astype(BF16)
        result(n, start)

    def when_chunk(n, f):
        @pl.when(jnp.logical_and(n >= 0, n < NC))
        def _():
            f(n)

    def step(i, c):
        @pl.when(jnp.logical_and(i >= 2, i - 2 < NC))
        def _():
            shared(i - 2, start)

        when_chunk(i, product)
        when_chunk(i, for_partner)
        when_chunk(i - 1, for_first)
        when_chunk(i, lambda n: to_partner(n, start))
        when_chunk(i - 2, for_second)
        when_chunk(i - 1, lambda n: first_hop(n, start))
        when_chunk(i - 3, for_own)
        when_chunk(i - 2, lambda n: second_hop(n, start))
        return c

    lax.fori_loop(0, NC + 3, step, 0)
    for n in (NC - 2, NC - 1):
        to_partner(n, wait_send)
        first_hop(n, wait_send)
        second_hop(n, wait_send)
        result(n, wait)


ANY = pl.BlockSpec(memory_space=pl.ANY)
VMEM_LIMIT = 67043328


def up(x, table, wg, wu, sg, su):
    dma = pltpu.SemaphoreType.DMA
    return pl.pallas_call(
        up_kernel,
        name="up",
        out_shape=(
            jax.ShapeDtypeStruct((N, T, D), BF16),
            jax.ShapeDtypeStruct((N, 2 * TOP, T), F32),
            jax.ShapeDtypeStruct((ROWS, FF), BF16),
            jax.ShapeDtypeStruct((T, FF), BF16),
        ),
        in_specs=[ANY] * 6,
        out_specs=(ANY,) * 4,
        scratch_shapes=[
            pltpu.VMEM((ROWS, FF), F32),
            pltpu.VMEM((ROWS, FF), F32),
            pltpu.VMEM((ROWS, KB), BF16),
            pltpu.VMEM((2, N, T, KB), BF16),
            pltpu.VMEM((WRING, 2, KB, FF), BF16),
            pltpu.VMEM((N, SEG, T), BF16),
            pltpu.VMEM((N, 2 * TOP, T), F32),
            dma((WRING, 2)),
            dma((3, N)),
            dma((4,)),
            dma((N - 1,)),
            dma((N - 1,)),
            dma((3, NK)),
            dma((3, NK)),
            dma((NK,)),
            dma((NK,)),
            dma((3, NK)),
            dma((3, NK)),
        ],
        compiler_params=pltpu.CompilerParams(collective_id=0, has_side_effects=True, vmem_limit_bytes=VMEM_LIMIT),
    )(x, table, wg, wu, sg, su)


def down(h, tables, wd, sh, sd):
    dma = pltpu.SemaphoreType.DMA
    return pl.pallas_call(
        down_kernel,
        name="down",
        out_shape=jax.ShapeDtypeStruct((T, D), BF16),
        in_specs=[ANY] * 5,
        out_specs=ANY,
        scratch_shapes=[
            pltpu.VMEM((ROWS, FF), BF16),
            pltpu.VMEM((DRING, FF, CB), BF16),
            pltpu.VMEM((2, FF, CB), BF16),
            pltpu.VMEM((T, FF), BF16),
            pltpu.VMEM((N, 2 * TOP, T), F32),
            pltpu.VMEM((N, T, -(-SEG // 128) * 128), BF16),
            pltpu.VMEM((4, N, SEG, CB), BF16),
            pltpu.VMEM((2, 4, T, CB), BF16),
            pltpu.VMEM((5, 4, T, CB), BF16),
            pltpu.VMEM((2, 2, 2, T, HB), BF16),
            pltpu.VMEM((NC, 2, 2, T, HB), BF16),
            pltpu.VMEM((2, 2, T, HB), BF16),
            pltpu.VMEM((NC, 2, T, HB), BF16),
            pltpu.VMEM((2, T, CB), BF16),
            dma((E,)),
            dma((DRING,)),
            dma((2,)),
            dma((2,)),
            dma((2,)),
            dma((2,)),
            dma((NC,)),
            dma((2, 2)),
            dma((NC, 2)),
            dma((2, 2)),
            dma((NC, 2)),
        ],
        compiler_params=pltpu.CompilerParams(collective_id=1, has_side_effects=True, vmem_limit_bytes=VMEM_LIMIT),
    )(h, tables, wd, sh, sd)


def solution(mesh):
    def device(x, expert, slot, gate, wg, wu, wd, sg, su, sd):
        key = jnp.where(slot < CAP, expert * CAP + slot, -1)[0, 0]
        weight = gate.astype(BF16)[0, 0]
        table = jnp.concatenate([key.T.astype(F32), weight.T.astype(F32)])
        _, tables, h, sh = up(x[0, 0], table, wg, wu, sg, su)
        return down(h, tables, wd, sh, sd)[None, None]

    tokens, experts = P("dp", "ep"), P("ep")
    return jax.shard_map(
        device,
        mesh=mesh,
        in_specs=(tokens,) * 4 + (experts,) * 3 + (P(),) * 3,
        out_specs=tokens,
        check_vma=False,
    )
```

```python
import functools

import jax
import jax.numpy as jnp
from jax import lax
from jax.experimental import pallas as pl
from jax.experimental.pallas import tpu as pltpu
from jax.sharding import PartitionSpec as P

MESH = pl.DeviceIdType.MESH
F32, BF16 = jnp.float32, jnp.bfloat16
N = 8
T = 256
D = 7168
FF = 2048
TOP = 8
E = 4
EXPERTS = N * E
CAP = 80
SEG = E * CAP
KB = 512
NK = D // KB
EARLY = 2
NB = 512
CB = 512
HB = CB // 2
NC = D // CB
SRING = 4
ROWS = 3 * TOP
FULL = (CAP,) * E
NARROW = (80, 80, 80, 32)
VMEM_LIMIT = 67043328

start, wait = (lambda c: c.start()), (lambda c: c.wait())
wait_send, wait_recv = (lambda c: c.wait_send()), (lambda c: c.wait_recv())


def around(me):
    i, j, c = me // 4, (me // 2) % 2, me % 2
    at = lambda i, j, c: i * 4 + j * 2 + c
    return at(i, j, 1 - c), at(1 - i, j, c), at(i, 1 - j, c), at(1 - i, 1 - j, c)


def greet(devices):
    barrier = pltpu.get_barrier_semaphore()
    for d in devices:
        pl.semaphore_signal(barrier, inc=1, device_id={"ep": d}, device_id_type=MESH)
    pl.semaphore_wait(barrier, len(devices))


def remote(src, dst, send, recv, to):
    return pltpu.make_async_remote_copy(
        src_ref=src, dst_ref=dst, send_sem=send, recv_sem=recv, device_id={"ep": to}, device_id_type=MESH
    )


def dot(a, b):
    return jnp.dot(a, b, preferred_element_type=F32)


def cols(k):
    return pl.ds(pl.multiple_of(k * KB, KB), KB)


class Way:
    def __init__(self, x, xg, sems):
        self.x, self.xg = x, xg
        self.o_send, self.o_recv, self.f_send, self.f_recv, self.c_send, self.c_recv = sems
        self.me = lax.axis_index("ep")
        self.cn, self.xn, self.yn, self.dg = around(self.me)

    def part(self, b, k):
        return self.xg.at[b, :, cols(k)]

    def own(self, k, run):
        for i, d in enumerate((self.xn, self.yn, self.cn)):
            run(remote(self.x.at[:, cols(k)], self.part(self.me, k), self.o_send.at[i, k], self.o_recv.at[i, k], d))

    def onward(self, k, run):
        p = lax.rem(k, 2)
        src, to = self.xn * (1 - p) + self.yn * p, self.yn * (1 - p) + self.xn * p
        run(remote(self.part(src, k), self.part(src, k), self.f_send.at[k], self.f_recv.at[k], to))

    def across(self, i, src, k, run):
        part = self.part(src, k)
        run(remote(part, part, self.c_send.at[i, k], self.c_recv.at[i, k], self.cn))

    def arrived(self, i, src, k):
        part = self.part(src, k)
        remote(part, part, self.o_send.at[i, k], self.o_recv.at[i, k], src).wait_recv()

    def forward(self, k):
        self.arrived(0, self.xn, k)
        self.arrived(1, self.yn, k)
        self.onward(k, start)
        self.across(0, self.xn, k, start)
        self.across(1, self.yn, k, start)

    def landed(self, k):
        part = self.part(self.dg, k)
        remote(part, part, self.f_send.at[k], self.f_recv.at[k], self.xn).wait_recv()

    def hand_over(self, k):
        self.landed(k)
        self.across(2, self.dg, k, start)

    def across_landed(self, i, k):
        part = self.part(self.cn, k)
        remote(part, part, self.c_send.at[i, k], self.c_recv.at[i, k], self.cn).wait_recv()

    def complete(self, k):
        self.arrived(2, self.cn, k)
        for i in range(3):
            self.across_landed(i, k)

    def passed_on(self, k, run):
        self.onward(k, run)
        for i, src in enumerate((self.xn, self.yn, self.dg)):
            self.across(i, src, k, run)


def way_semaphores(chunks):
    dma = pltpu.SemaphoreType.DMA
    return [dma((3, chunks)), dma((3, chunks)), dma((chunks,)), dma((chunks,)), dma((3, chunks)), dma((3, chunks))]


def share_kernel(
    expert, slot, gate, x, sg, su, xg, tables, plan, sh,
    mine, tv, pv, xv, wv, acc_g, acc_u, hv, x_sem, w_sem, h_sem, t_send, t_recv, *sems,
):
    me = lax.axis_index("ep")
    others = [lax.rem(me + d, N) for d in range(1, N)]
    way = Way(x, xg, sems)

    def weights(s, run):
        at = lax.rem(s, SRING)
        for half, ref in ((0, sg), (1, su)):
            run(pltpu.make_async_copy(ref.at[cols(s)], wv.at[at, half], w_sem.at[at, half]))

    def tokens(s, run):
        run(pltpu.make_async_copy(x.at[:, cols(s)], xv.at[s], x_sem.at[s]))

    for s in range(SRING - 1):
        tokens(s, start)
        weights(s, start)

    key = jnp.where(slot[...] < CAP, expert[...] * CAP + slot[...], -1).astype(F32)
    mine[:TOP] = key
    mine[TOP:2 * TOP] = gate[...].astype(BF16).astype(F32)
    key = jnp.concatenate([key, jnp.zeros((128 - TOP, T), F32)]).T
    low = (lax.broadcasted_iota(jnp.int32, (T, 128), 1) * CAP).astype(F32)
    used = jnp.zeros((T, 128), F32)
    for j in range(TOP):
        depth = key[:, j:j + 1] - low
        used = jnp.maximum(used, jnp.where((depth >= 0) & (depth < CAP), depth + 1, 0.0))
    used = jnp.max(used, axis=0, keepdims=True)
    mine[2 * TOP:] = jnp.broadcast_to(jnp.concatenate([used, used], axis=1), (TOP, T))

    greet(others)
    for k in range(EARLY):
        way.own(k, start)
    for i, d in enumerate(others):
        remote(mine, tv.at[me], t_send.at[i], t_recv.at[N - 2 - i], d).start()
    for s in range(SRING - 1, NK):
        tokens(s, start)
    tv[me] = mine[...]

    def step(s, first):
        @pl.when(s + SRING - 1 < NK)
        def _():
            weights(s + SRING - 1, start)

        tokens(s, wait)
        weights(s, wait)
        for n in range(FF // NB):
            b = slice(n * NB, (n + 1) * NB)
            for half, acc in ((0, acc_g), (1, acc_u)):
                v = dot(xv[s], wv[lax.rem(s, SRING), half, :, b])
                acc[:, b] = v if first else acc[:, b] + v

    step(0, True)

    def body(s, c):
        step(s, False)

        @pl.when(s == 5)
        def _():
            way.forward(0)

        @pl.when(s == 9)
        def _():
            way.forward(1)

        return c

    lax.fori_loop(1, NK, body, 0)
    for i in range(N - 1):
        b = lax.rem(me + 1 + i, N)
        remote(mine, tv.at[b], t_send.at[i], t_recv.at[i], b).wait_recv()
    keep = pltpu.make_async_copy(tv, tables, h_sem.at[0])
    keep.start()
    way.hand_over(0)

    n = tv[0, 2 * TOP:, :128]
    for b in range(1, N):
        n = jnp.maximum(n, tv[b, 2 * TOP:, :128])
    lane = lax.broadcasted_iota(jnp.int32, n.shape, 1)
    e = lane % E
    rank = jnp.zeros(n.shape, jnp.int32)
    for o in range(1, E):
        later = e + o < E
        other = jnp.where(later, pltpu.roll(n, 128 - o, 1), pltpu.roll(n, E - o, 1))
        rank = rank + ((other > n) | ((other == n) & jnp.logical_not(later))).astype(jnp.int32)
    caps = jnp.zeros(n.shape, F32)
    for r in range(E):
        caps = jnp.where(rank == r, float(NARROW[r]), caps)
    over = jnp.where((n > caps) & (lane < EXPERTS), 1.0, 0.0)
    out = jnp.where(lane == E, jnp.max(over, axis=1, keepdims=True), 0.0)
    for r in range(E):
        chosen = jnp.where((lane // E == me) & (rank == r), e, 0).astype(F32)
        out = out + jnp.where(lane == r, jnp.sum(chosen, axis=1, keepdims=True), 0.0)
    pv[...] = out.astype(jnp.int32)

    hv[...] = (jax.nn.silu(acc_g[...]) * acc_u[...]).astype(BF16)
    keep_plan = pltpu.make_async_copy(pv, plan, h_sem.at[2])
    keep_plan.start()
    keep_sh = pltpu.make_async_copy(hv, sh, h_sem.at[1])
    keep_sh.start()
    for i, d in enumerate(others):
        remote(mine, tv.at[me], t_send.at[i], t_recv.at[N - 2 - i], d).wait_send()
    way.complete(0)
    way.across(2, way.dg, 0, wait_send)
    way.arrived(2, way.cn, 1)
    way.landed(1)
    for k in range(EARLY):
        way.own(k, wait_send)
        way.onward(k, wait_send)
        for i, src in enumerate((way.xn, way.yn)):
            way.across(i, src, k, wait_send)
    for i in range(2):
        way.across_landed(i, 1)
    keep.wait()
    keep_plan.wait()
    keep_sh.wait()


def bases(caps):
    return [sum(caps[:r]) for r in range(E)]


def ranks(caps, plan):
    return list(range(E)) if caps == FULL else [plan[0, r] for r in range(E)]


def up_kernel(
    caps, plan, x, _, tables, wg, wu, xg, h, acc_g, acc_u, z, xv, w0, w1, pick, tv, w_sem, x_sem, z_sem, t_sem, *sems
):
    seg, at = sum(caps), bases(caps)
    wv = (w0, w1)
    width = w0.shape[-1]
    parts = FF // width
    me = lax.axis_index("ep")
    way = Way(x, xg, sems)
    perm = ranks(caps, plan)

    def weights(s, slot, run):
        @pl.when(s < NK * parts)
        def _():
            k, lanes = s // parts, pl.ds(pl.multiple_of(lax.rem(s, parts) * width, width), width)
            for e in range(E):
                for half, ref in ((0, wg), (1, wu)):
                    run(pltpu.make_async_copy(ref.at[e, cols(k), lanes], wv[slot].at[e, half], w_sem.at[slot, e, half]))

    def tokens(k, run):
        slot = lax.rem(k, 2)

        @pl.when(k < NK)
        def _():
            for d in range(1, N):
                b = lax.rem(me + d, N)
                run(pltpu.make_async_copy(way.part(b, k), xv.at[slot, b], x_sem.at[slot, b]))
            run(pltpu.make_async_copy(x.at[:, cols(k)], xv.at[slot, me], x_sem.at[slot, me]))

    load_tables = pltpu.make_async_copy(tables, tv, t_sem)
    load_tables.start()
    tokens(0, start)
    weights(0, 0, start)
    greet((way.cn, way.xn, way.yn))
    way.across(2, way.dg, EARLY - 1, start)
    for k in range(EARLY, EARLY + 2):
        way.own(k, start)

    load_tables.wait()
    first_key = [(me * E + perm[r]) * CAP for r in range(E)]

    def picks(b, c):
        for r in range(E):
            key = (lax.broadcasted_iota(jnp.int32, (caps[r], T), 0) + first_key[r]).astype(F32)
            hit = jnp.zeros((caps[r], T), F32)
            for j in range(TOP):
                hit = hit + jnp.where(tv[b, j:j + 1, :] == key, 1.0, 0.0)
            pick[b, at[r]:at[r] + caps[r]] = hit.astype(BF16)
        return c

    lax.fori_loop(0, N, picks, 0)

    def clear(i, c):
        rows = pl.ds(pl.multiple_of(i * 16, 16), 16)
        acc_g[rows] = jnp.zeros((16, FF), F32)
        acc_u[rows] = jnp.zeros((16, FF), F32)
        return c

    lax.fori_loop(0, N * seg // 16, clear, 0)

    def gather(k):
        slot = lax.rem(k, 2)
        tokens(k, wait)
        for b in range(N):
            v = dot(pick[b], xv[slot, b]).astype(BF16)
            for r in range(E):
                z[N * at[r] + b * caps[r]:N * at[r] + (b + 1) * caps[r]] = v[at[r]:at[r] + caps[r]]

    def product(k, j, slot):
        s = k * parts + j
        weights(s + 1, 1 - slot, start)
        weights(s, slot, wait)
        for n in range(width // NB):
            b = pl.ds(pl.multiple_of(j * width + n * NB, NB), NB)
            for r in range(E):
                rows = slice(N * at[r], N * (at[r] + caps[r]))
                for half, acc in ((0, acc_g), (1, acc_u)):
                    acc[rows, b] = acc[rows, b] + dot(
                        z[rows], wv[slot][perm[r], half, :, n * NB:(n + 1) * NB]
                    )

    def bring(k):
        @pl.when(k < NK)
        def _():
            @pl.when(k >= EARLY)
            def _():
                way.complete(k)

            @pl.when(k == EARLY - 1)
            def _():
                way.across_landed(2, k)

            tokens(k, start)

    def middle(k):
        @pl.when(k == 0)
        def _():
            way.forward(EARLY)

        @pl.when(k + 4 < NK)
        def _():
            way.own(k + 4, start)

        bring(k + 1)

    def end(k):
        @pl.when(k + 3 < NK)
        def _():
            way.forward(k + 3)

        @pl.when(k + 2 < NK)
        def _():
            way.hand_over(k + 2)

    def chunk(k, c):
        gather(k)

        half = parts // 2 - 1

        def pair(i, c):
            for slot in range(2):
                product(k, 2 * i + slot, slot)
                if slot == half % 2:
                    pl.when(i == half // 2)(lambda: middle(k))
            return c

        lax.fori_loop(0, parts // 2, pair, 0)
        end(k)
        return c

    lax.fori_loop(0, NK, chunk, 0)

    def store(n, r, run):
        rows = slice(N * at[r], N * (at[r] + caps[r]))
        run(pltpu.make_async_copy(z.at[rows], h.at[rows, pl.ds(pl.multiple_of(n * KB, KB), KB)], z_sem.at[r]))

    def finish(n, c):
        lanes = pl.ds(pl.multiple_of(n * KB, KB), KB)
        for r in range(E):
            rows = slice(N * at[r], N * (at[r] + caps[r]))

            @pl.when(n > 0)
            def _():
                store(n - 1, r, wait)

            z[rows] = (jax.nn.silu(acc_g[rows, lanes]) * acc_u[rows, lanes]).astype(BF16)
            store(n, r, start)
        return c

    lax.fori_loop(0, FF // KB, finish, 0)
    for r in range(E):
        store(FF // KB - 1, r, wait)

    way.across(2, way.dg, EARLY - 1, wait_send)

    def drain(k, c):
        way.own(k, wait_send)
        way.passed_on(k, wait_send)
        return c

    lax.fori_loop(EARLY, NK, drain, 0)


def down_kernel(
    caps, plan, h, tables, wd, sh, sd, y,
    hv, w0, w1, sv, shv, tv, comb, out, d_out, d_in, p_out, p_in, q_out, q_in, part, own, yv,
    h_sem, w_sem, s_sem, m_sem, y_sem, d_send, d_recv, p_send, p_recv, q_send, q_recv,
):
    seg, at = sum(caps), bases(caps)
    me = lax.axis_index("ep")
    cn, xn, yn, dg = around(me)
    perm = ranks(caps, plan)

    def lanes(n):
        return pl.ds(pl.multiple_of(n * CB, CB), CB)

    def buffer(slot):
        return w0.at[slot] if caps == FULL else (w0, w1)[slot]

    def weights(n, slot, run):
        for e in range(E):
            run(pltpu.make_async_copy(wd.at[e, :, lanes(n)], buffer(slot).at[e], w_sem.at[slot, e]))

    def each_slot(n, f):
        if caps == FULL:
            f(lax.rem(n, 2))
        else:
            for slot in range(2):
                pl.when(lax.rem(n, 2) == slot)(functools.partial(f, slot))

    def shared(n, run):
        slot = lax.rem(n, 2)
        run(pltpu.make_async_copy(sd.at[:, lanes(n)], sv.at[slot], s_sem.at[slot]))

    def activations(r, run):
        rows = slice(N * at[r], N * (at[r] + caps[r]))
        run(pltpu.make_async_copy(h.at[rows], hv.at[rows], h_sem.at[r]))

    for r in range(E):
        activations(r, start)
    weights(0, 0, start)
    load_tables = pltpu.make_async_copy(tables, tv, m_sem.at[0])
    load_tables.start()
    load_sh = pltpu.make_async_copy(sh, shv, m_sem.at[1])
    load_sh.start()
    shared(0, start)
    greet((cn, xn, yn))

    def product(slot, r):
        v = dot(hv[N * at[r]:N * (at[r] + caps[r])], buffer(slot)[perm[r]]).astype(BF16)
        for b in range(N):
            out[slot, b, at[r]:at[r] + caps[r]] = v[b * caps[r]:(b + 1) * caps[r]]

    def combines():
        load_tables.wait()
        wide = comb.shape[-1]

        def one(b, c):
            v = []
            for r in range(E):
                key = (lax.broadcasted_iota(jnp.int32, (caps[r], T), 0) + (me * E + perm[r]) * CAP).astype(F32)
                w = jnp.zeros((caps[r], T), F32)
                for j in range(TOP):
                    w = w + jnp.where(tv[b, j:j + 1, :] == key, tv[b, TOP + j:TOP + j + 1, :], 0.0)
                v.append(w)
            v.append(jnp.zeros((wide - seg, T), F32))
            comb[b] = jnp.concatenate(v).T.astype(BF16)
            return c

        lax.fori_loop(0, N, one, 0)
        load_sh.wait()

    def summed(b, n):
        return dot(comb[b][:, :seg], out[lax.rem(n, 2), b])

    left, right = slice(0, HB), slice(HB, CB)

    def to_partner(n, run):
        slot = lax.rem(n, 2)
        run(remote(d_out.at[slot], d_in.at[slot], d_send.at[slot], d_recv.at[n], cn))

    def first_hop(n, run):
        slot = lax.rem(n, 2)
        for i, d in enumerate((xn, yn)):
            run(remote(p_out.at[slot, i], p_in.at[lax.rem(n, 6), i], p_send.at[slot, i], p_recv.at[n, i], d))

    def second_hop(n, run):
        slot = lax.rem(n, 2)
        for i, d in enumerate((yn, xn)):
            run(remote(q_out.at[slot, i], q_in.at[lax.rem(n, 4), i], q_send.at[slot, i], q_recv.at[n, i], d))

    def result(n, run):
        slot = lax.rem(n, 2)
        run(pltpu.make_async_copy(yv.at[slot], y.at[:, lanes(n)], y_sem.at[slot]))

    def for_partner(n, slot):
        for i, b in enumerate((cn,) + around(cn)[1:]):
            d_out[slot, i] = dot(comb[b][:, :seg], out[slot, b]).astype(BF16)

    def for_first(n):
        slot = lax.rem(n, 2)
        v = [summed(b, n) + d_in[slot, i].astype(F32) for i, b in ((3, dg), (1, xn), (2, yn), (0, me))]
        p_out[slot, 0, 1] = v[0][:, left].astype(BF16)
        p_out[slot, 1, 1] = v[0][:, right].astype(BF16)
        p_out[slot, 0, 0] = v[1][:, left].astype(BF16)
        part[lax.rem(n, 3), 1] = v[1][:, right]
        p_out[slot, 1, 0] = v[2][:, right].astype(BF16)
        part[lax.rem(n, 3), 0] = v[2][:, left]
        own[lax.rem(n, 5)] = v[3]

    def for_second(n):
        for i in range(2):
            q_out[lax.rem(n, 2), i] = (part[lax.rem(n, 3), i] + p_in[lax.rem(n, 6), i, 1].astype(F32)).astype(BF16)

    def for_own(n):
        v = own[lax.rem(n, 5)] + dot(shv[...], sv[lax.rem(n, 2)])
        for i, half in enumerate((left, right)):
            w = v[:, half] + p_in[lax.rem(n, 6), i, 0].astype(F32) + q_in[lax.rem(n, 4), i].astype(F32)
            yv[lax.rem(n, 2), :, half] = w.astype(BF16)

    def ready_first(n):
        @pl.when(n >= 2)
        def _():
            first_hop(n - 2, wait_send)

        to_partner(n, wait_recv)

    def ready_second(n):
        @pl.when(n >= 2)
        def _():
            second_hop(n - 2, wait_send)

        first_hop(n, wait_recv)

    def ready_own(n):
        @pl.when(n >= 2)
        def _():
            result(n - 2, wait)

        shared(n, wait)
        second_hop(n, wait_recv)

    stages = (
        (1, ready_first, for_first, first_hop),
        (3, ready_second, for_second, second_hop),
        (5, ready_own, for_own, result),
    )

    def step(i, c):
        @pl.when(i + 1 < NC)
        def _():
            each_slot(i + 1, lambda slot: weights(i + 1, slot, start))

        @pl.when(jnp.logical_and(i >= 5, i - 4 < NC))
        def _():
            shared(i - 4, start)

        @pl.when(i == 0)
        def _():
            for r in range(E):
                activations(r, wait)

        @pl.when(i < NC)
        def _():
            def half(slot):
                weights(i, slot, wait)
                for r in range(E // 2):
                    product(slot, r)

            each_slot(i, half)

        inner = jnp.logical_and(i >= 5, i <= NC)

        @pl.when(inner)
        def _():
            for lag, ready, _, _ in stages:
                ready(i - lag)
            for lag, _, compute, _ in stages:
                compute(i - lag)
            for lag, _, _, go in stages:
                go(i - lag, start)

        @pl.when(jnp.logical_not(inner))
        def _():
            for lag, ready, compute, go in stages:
                n = i - lag

                @pl.when(jnp.logical_and(n >= 0, n < NC))
                def _():
                    ready(n)
                    compute(n)
                    go(n, start)

        @pl.when(i == 0)
        def _():
            combines()

        @pl.when(i < NC)
        def _():
            @pl.when(i >= 2)
            def _():
                to_partner(i - 2, wait_send)

            def half(slot):
                for r in range(E // 2, E):
                    product(slot, r)
                for_partner(i, slot)

            each_slot(i, half)
            to_partner(i, start)

        return c

    lax.fori_loop(0, NC + 5, step, 0)
    for n in (NC - 2, NC - 1):
        to_partner(n, wait_send)
        first_hop(n, wait_send)
        second_hop(n, wait_send)
        result(n, wait)


ANY = pl.BlockSpec(memory_space=pl.ANY)
SMEM = pl.BlockSpec(memory_space=pltpu.SMEM)
DMA = pltpu.SemaphoreType.DMA


def params(i):
    return pltpu.CompilerParams(collective_id=i, has_side_effects=True, vmem_limit_bytes=VMEM_LIMIT)


def share(expert, slot, gate, x, sg, su):
    return pl.pallas_call(
        share_kernel,
        name="share",
        out_shape=(
            jax.ShapeDtypeStruct((N, T, D), BF16),
            jax.ShapeDtypeStruct((N, ROWS, T), F32),
            jax.ShapeDtypeStruct((TOP, 128), jnp.int32),
            jax.ShapeDtypeStruct((T, FF), BF16),
        ),
        in_specs=[pl.BlockSpec(memory_space=pltpu.VMEM)] * 3 + [ANY] * 3,
        out_specs=(ANY,) * 4,
        scratch_shapes=[
            pltpu.VMEM((ROWS, T), F32),
            pltpu.VMEM((N, ROWS, T), F32),
            pltpu.VMEM((TOP, 128), jnp.int32),
            pltpu.VMEM((NK, T, KB), BF16),
            pltpu.VMEM((SRING, 2, KB, FF), BF16),
            pltpu.VMEM((T, FF), F32),
            pltpu.VMEM((T, FF), F32),
            pltpu.VMEM((T, FF), BF16),
            DMA((NK,)),
            DMA((SRING, 2)),
            DMA((3,)),
            DMA((N - 1,)),
            DMA((N - 1,)),
        ]
        + way_semaphores(EARLY),
        compiler_params=params(0),
    )(expert, slot, gate, x, sg, su)


def up(caps, width, identity, plan, x, xg, tables, wg, wu):
    seg = sum(caps)
    return pl.pallas_call(
        functools.partial(up_kernel, caps),
        name="up",
        out_shape=(jax.ShapeDtypeStruct((N, T, D), BF16), jax.ShapeDtypeStruct((N * seg, FF), BF16)),
        input_output_aliases={2: 0},
        in_specs=[SMEM] + [ANY] * 5,
        out_specs=(ANY,) * 2,
        scratch_shapes=[
            pltpu.VMEM((N * seg, FF), F32),
            pltpu.VMEM((N * seg, FF), F32),
            pltpu.VMEM((N * seg, KB), BF16),
            pltpu.VMEM((2, N, T, KB), BF16),
            pltpu.VMEM((E, 2, KB, width), BF16),
            pltpu.VMEM((E, 2, KB, width), BF16),
            pltpu.VMEM((N, seg, T), BF16),
            pltpu.VMEM((N, ROWS, T), F32),
            DMA((2, E, 2)),
            DMA((2, N)),
            DMA((E,)),
            DMA,
        ]
        + way_semaphores(NK),
        compiler_params=params(identity),
    )(plan, x, xg, tables, wg, wu)[1]


def down(caps, identity, plan, h, tables, wd, sh, sd):
    seg = sum(caps)
    return pl.pallas_call(
        functools.partial(down_kernel, caps),
        name="down",
        out_shape=jax.ShapeDtypeStruct((T, D), BF16),
        in_specs=[SMEM] + [ANY] * 5,
        out_specs=ANY,
        scratch_shapes=[
            pltpu.VMEM((N * seg, FF), BF16),
            pltpu.VMEM((2, E, FF, CB) if caps == FULL else (E, FF, CB), BF16),
            pltpu.VMEM((16, 128) if caps == FULL else (E, FF, CB), BF16),
            pltpu.VMEM((2, FF, CB), BF16),
            pltpu.VMEM((T, FF), BF16),
            pltpu.VMEM((N, ROWS, T), F32),
            pltpu.VMEM((N, T, -(-seg // 128) * 128), BF16),
            pltpu.VMEM((2, N, seg, CB), BF16),
            pltpu.VMEM((2, 4, T, CB), BF16),
            pltpu.VMEM((2, 4, T, CB), BF16),
            pltpu.VMEM((2, 2, 2, T, HB), BF16),
            pltpu.VMEM((6, 2, 2, T, HB), BF16),
            pltpu.VMEM((2, 2, T, HB), BF16),
            pltpu.VMEM((4, 2, T, HB), BF16),
            pltpu.VMEM((3, 2, T, HB), F32),
            pltpu.VMEM((5, T, CB), F32),
            pltpu.VMEM((2, T, CB), BF16),
            DMA((E,)),
            DMA((2, E)),
            DMA((2,)),
            DMA((2,)),
            DMA((2,)),
            DMA((2,)),
            DMA((NC,)),
            DMA((2, 2)),
            DMA((NC, 2)),
            DMA((2, 2)),
            DMA((NC, 2)),
        ],
        compiler_params=params(identity),
    )(plan, h, tables, wd, sh, sd)


def solution(mesh):
    def device(x, expert, slot, gate, wg, wu, wd, sg, su, sd):
        x, expert, slot, gate = x[0, 0], expert[0, 0], slot[0, 0], gate[0, 0]
        xg, tables, plan, sh = share(expert.T, slot.T, gate.T, x, sg, su)

        def experts(caps, width, identity):
            h = up(caps, width, identity, plan, x, xg, tables, wg, wu)
            return down(caps, identity + 1, plan, h, tables, wd, sh, sd)

        y = lax.cond(plan[0, E] == 0, lambda: experts(NARROW, 1024, 1), lambda: experts(FULL, 512, 3))
        return y[None, None]

    tokens, experts = P("dp", "ep"), P("ep")
    return jax.shard_map(
        device,
        mesh=mesh,
        in_specs=(tokens,) * 4 + (experts,) * 3 + (P(),) * 3,
        out_specs=tokens,
        check_vma=False,
    )
```

```python
import functools

import jax
import jax.numpy as jnp
from jax import lax
from jax.experimental import pallas as pl
from jax.experimental.pallas import tpu as pltpu
from jax.sharding import PartitionSpec as P

MESH = pl.DeviceIdType.MESH
F32, BF16 = jnp.float32, jnp.bfloat16
N = 8
T = 256
D = 7168
FF = 2048
TOP = 8
E = 4
EXPERTS = N * E
CAP = 80
SEG = E * CAP
KB = 512
NK = D // KB
EARLY = 2
NB = 512
CB = 512
HB = CB // 2
NC = D // CB
SRING = 4
ROWS = 3 * TOP
FULL = (CAP,) * E
NARROW = (80, 80, 80, 32)
VMEM_LIMIT = 67043328

start, wait = (lambda c: c.start()), (lambda c: c.wait())
wait_send, wait_recv = (lambda c: c.wait_send()), (lambda c: c.wait_recv())


def around(me):
    i, j, c = me // 4, (me // 2) % 2, me % 2
    at = lambda i, j, c: i * 4 + j * 2 + c
    return at(i, j, 1 - c), at(1 - i, j, c), at(i, 1 - j, c), at(1 - i, 1 - j, c)


def greet(devices):
    barrier = pltpu.get_barrier_semaphore()
    for d in devices:
        pl.semaphore_signal(barrier, inc=1, device_id={"ep": d}, device_id_type=MESH)
    pl.semaphore_wait(barrier, len(devices))


def remote(src, dst, send, recv, to):
    return pltpu.make_async_remote_copy(
        src_ref=src, dst_ref=dst, send_sem=send, recv_sem=recv, device_id={"ep": to}, device_id_type=MESH
    )


def dot(a, b):
    return jnp.dot(a, b, preferred_element_type=F32)


def cols(k):
    return pl.ds(pl.multiple_of(k * KB, KB), KB)


class Way:
    def __init__(self, x, xg, sems):
        self.x, self.xg = x, xg
        self.o_send, self.o_recv, self.f_send, self.f_recv, self.c_send, self.c_recv = sems
        self.me = lax.axis_index("ep")
        self.cn, self.xn, self.yn, self.dg = around(self.me)

    def part(self, b, k):
        return self.xg.at[b, :, cols(k)]

    def own(self, k, run):
        for i, d in enumerate((self.xn, self.yn, self.cn)):
            run(remote(self.x.at[:, cols(k)], self.part(self.me, k), self.o_send.at[i, k], self.o_recv.at[i, k], d))

    def half(self, b, k, i):
        return self.xg.at[b, :, pl.ds(pl.multiple_of(k * KB + i * (KB // 2), KB // 2), KB // 2)]

    def onward(self, k, run):
        for i, (src, to) in enumerate(((self.xn, self.yn), (self.yn, self.xn))):
            part = self.half(src, k, i)
            run(remote(part, part, self.f_send.at[i, k], self.f_recv.at[i, k], to))

    def across(self, i, src, k, run):
        part = self.part(src, k)
        run(remote(part, part, self.c_send.at[i, k], self.c_recv.at[i, k], self.cn))

    def arrived(self, i, src, k):
        part = self.part(src, k)
        remote(part, part, self.o_send.at[i, k], self.o_recv.at[i, k], src).wait_recv()

    def forward(self, k):
        self.arrived(0, self.xn, k)
        self.arrived(1, self.yn, k)
        self.pass_on(k)

    def pass_on(self, k):
        self.onward(k, start)
        self.across(0, self.xn, k, start)
        self.across(1, self.yn, k, start)

    def landed(self, k):
        for i, src in enumerate((self.yn, self.xn)):
            part = self.half(self.dg, k, i)
            remote(part, part, self.f_send.at[i, k], self.f_recv.at[i, k], src).wait_recv()

    def hand_over(self, k):
        self.landed(k)
        self.across(2, self.dg, k, start)

    def complete(self, k):
        self.arrived(2, self.cn, k)
        self.crossed(k)

    def crossed(self, k):
        for i in range(3):
            part = self.part(self.cn, k)
            remote(part, part, self.c_send.at[i, k], self.c_recv.at[i, k], self.cn).wait_recv()

    def drain(self, k):
        self.onward(k, wait_send)
        for i, src in enumerate((self.xn, self.yn, self.dg)):
            self.across(i, src, k, wait_send)


def way_semaphores(chunks):
    dma = pltpu.SemaphoreType.DMA
    return [dma((3, chunks)), dma((3, chunks)), dma((2, chunks)), dma((2, chunks)), dma((3, chunks)), dma((3, chunks))]


def share_kernel(
    expert, slot, gate, x, sg, su, xg, tables, picks, plan, wide, sh,
    mine, tv, pv, pick, xv, wv, acc_g, acc_u, hv, x_sem, w_sem, h_sem, t_send, t_recv, *sems,
):
    me = lax.axis_index("ep")
    others = [lax.rem(me + d, N) for d in range(1, N)]
    way = Way(x, xg, sems)

    def weights(s, run):
        at = lax.rem(s, SRING)
        for half, ref in ((0, sg), (1, su)):
            run(pltpu.make_async_copy(ref.at[cols(s)], wv.at[at, half], w_sem.at[at, half]))

    def tokens(s, run):
        run(pltpu.make_async_copy(x.at[:, cols(s)], xv.at[s], x_sem.at[s]))

    for s in range(SRING - 1):
        tokens(s, start)
        weights(s, start)

    key = jnp.where(slot[...] < CAP, expert[...] * CAP + slot[...], -1).astype(F32)
    mine[:TOP] = key
    mine[TOP:2 * TOP] = gate[...].astype(BF16).astype(F32)
    key = jnp.concatenate([key, jnp.zeros((128 - TOP, T), F32)]).T
    low = (lax.broadcasted_iota(jnp.int32, (T, 128), 1) * CAP).astype(F32)
    used = jnp.zeros((T, 128), F32)
    for j in range(TOP):
        depth = key[:, j:j + 1] - low
        used = jnp.maximum(used, jnp.where((depth >= 0) & (depth < CAP), depth + 1, 0.0))
    used = jnp.max(used, axis=0, keepdims=True)
    mine[2 * TOP:] = jnp.broadcast_to(jnp.concatenate([used, used], axis=1), (TOP, T))

    greet(others)
    for i, d in enumerate(others):
        remote(mine, tv.at[me], t_send.at[i], t_recv.at[N - 2 - i], d).start()
    for k in range(EARLY):
        way.own(k, start)
    for s in range(SRING - 1, NK):
        tokens(s, start)
    tv[me] = mine[...]

    def project(s):
        for n in range(FF // NB):
            b = slice(n * NB, (n + 1) * NB)
            for half, acc in ((0, acc_g), (1, acc_u)):
                acc[:, b] = acc[:, b] + dot(xv[s], wv[lax.rem(s, SRING), half, :, b])

    def ready(s):
        @pl.when(s + SRING - 1 < NK)
        def _():
            weights(s + SRING - 1, start)

        tokens(s, wait)
        weights(s, wait)

    acc_g[...] = jnp.zeros((T, FF), F32)
    acc_u[...] = jnp.zeros((T, FF), F32)

    def first_steps(s, c):
        ready(s)
        project(s)
        return c

    lax.fori_loop(0, NK - N - 1, first_steps, 0)
    for i, b in enumerate(others):
        remote(mine, tv.at[b], t_send.at[i], t_recv.at[i], b).wait_recv()
    keep = pltpu.make_async_copy(tv, tables, h_sem.at[0])
    keep.start()

    row = (lax.broadcasted_iota(jnp.int32, (SEG, T), 0) + me * SEG).astype(F32)

    def last_steps(s, c):
        ready(s)
        b = jnp.minimum(s - (NK - N - 1), N - 1)
        hit = tv[b, :1, :] == row
        for j in range(1, TOP):
            hit = hit | (tv[b, j:j + 1, :] == row)
        hit = jnp.where(hit, 1.0, 0.0).astype(BF16)
        for e in range(E):
            pick[b, e] = hit[e * CAP:(e + 1) * CAP]
        project(s)

        @pl.when(s == 6)
        def _():
            way.forward(0)

        @pl.when(s == 9)
        def _():
            way.forward(1)
            way.own(2, start)

        @pl.when(s == 12)
        def _():
            way.hand_over(0)

        return c

    lax.fori_loop(NK - N - 1, NK, last_steps, 0)
    keep_picks = pltpu.make_async_copy(pick, picks, h_sem.at[3])
    keep_picks.start()
    way.hand_over(1)

    n = tv[0, 2 * TOP:, :128]
    for b in range(1, N):
        n = jnp.maximum(n, tv[b, 2 * TOP:, :128])
    lane = lax.broadcasted_iota(jnp.int32, n.shape, 1)
    e = lane % E
    rank = jnp.zeros(n.shape, jnp.int32)
    for o in range(1, E):
        later = e + o < E
        other = jnp.where(later, pltpu.roll(n, 128 - o, 1), pltpu.roll(n, E - o, 1))
        rank = rank + ((other > n) | ((other == n) & jnp.logical_not(later))).astype(jnp.int32)
    caps = jnp.zeros(n.shape, F32)
    for r in range(E):
        caps = jnp.where(rank == r, float(NARROW[r]), caps)
    wide[0] = jnp.max(jnp.where((n > caps) & (lane < EXPERTS), 1.0, 0.0)).astype(jnp.int32)
    out = jnp.zeros(n.shape, F32)
    for r in range(E):
        chosen = jnp.where((lane // E == me) & (rank == r), e, 0).astype(F32)
        out = out + jnp.where(lane == r, jnp.sum(chosen, axis=1, keepdims=True), 0.0)
    pv[...] = out.astype(jnp.int32)

    hv[...] = (jax.nn.silu(acc_g[...]) * acc_u[...]).astype(BF16)
    keep_plan = pltpu.make_async_copy(pv, plan, h_sem.at[2])
    keep_plan.start()
    keep_sh = pltpu.make_async_copy(hv, sh, h_sem.at[1])
    keep_sh.start()
    for i, d in enumerate(others):
        remote(mine, tv.at[me], t_send.at[i], t_recv.at[N - 2 - i], d).wait_send()
    for k in range(EARLY):
        way.complete(k)
        way.own(k, wait_send)
        way.drain(k)
    for i, src in enumerate((way.xn, way.yn, way.cn)):
        way.arrived(i, src, EARLY)
    way.own(EARLY, wait_send)
    keep.wait()
    keep_plan.wait()
    keep_picks.wait()
    keep_sh.wait()


def buffers(caps, w0, w1):
    full = caps == FULL
    buffer = lambda slot: w0.at[slot] if full else (w0, w1)[slot]

    def in_slot(slot, f):
        if full or isinstance(slot, int):
            f(slot)
        else:
            for q in range(2):
                pl.when(slot == q)(functools.partial(f, q))

    return buffer, in_slot


def bases(caps):
    return [sum(caps[:r]) for r in range(E)]


def ranks(caps, plan):
    return list(range(E)) if caps == FULL else [plan[0, r] for r in range(E)]


def up_kernel(
    caps, plan, x, _, picks, wg, wu, xg, h, acc_g, acc_u, z, xv, w0, w1, pick, w_sem, x_sem, z_sem, p_sem, *sems
):
    seg, at = sum(caps), bases(caps)
    width = w0.shape[-1]
    parts = FF // width
    me = lax.axis_index("ep")
    way = Way(x, xg, sems)
    perm = ranks(caps, plan)
    buffer, in_slot = buffers(caps, w0, w1)

    def weights(s, run):
        def copies(slot):
            k, lanes = s // parts, pl.ds(pl.multiple_of(lax.rem(s, parts) * width, width), width)
            for e in range(E):
                for half, ref in ((0, wg), (1, wu)):
                    run(pltpu.make_async_copy(ref.at[e, cols(k), lanes], buffer(slot).at[e, half], w_sem.at[slot, e, half]))

        pl.when(s < NK * parts)(lambda: in_slot(lax.rem(s, 2), copies))

    def tokens(k, run):
        slot = lax.rem(k, 2)

        @pl.when(k < NK)
        def _():
            for d in range(1, N):
                b = lax.rem(me + d, N)
                run(pltpu.make_async_copy(way.part(b, k), xv.at[slot, b], x_sem.at[slot, b]))
            run(pltpu.make_async_copy(x.at[:, cols(k)], xv.at[slot, me], x_sem.at[slot, me]))

    load_picks = pltpu.make_async_copy(picks, pick, p_sem)
    load_picks.start()
    tokens(0, start)
    weights(0, start)
    tokens(1, start)
    greet((way.cn, way.xn, way.yn))
    way.pass_on(EARLY)
    way.own(EARLY + 1, start)
    way.own(EARLY + 2, start)

    def clear(i, c):
        rows = pl.ds(pl.multiple_of(i * 64, 64), 64)
        acc_g[rows] = jnp.zeros((64, FF), F32)
        acc_u[rows] = jnp.zeros((64, FF), F32)
        return c

    lax.fori_loop(0, N * seg // 64, clear, 0)
    load_picks.wait()

    def gather(k):
        slot = lax.rem(k, 2)
        tokens(k, wait)
        for b in range(N):
            hit = jnp.concatenate([pick[b, perm[r]][:caps[r]] for r in range(E)])
            v = dot(hit, xv[slot, b]).astype(BF16)
            for r in range(E):
                z[N * at[r] + b * caps[r]:N * at[r] + (b + 1) * caps[r]] = v[at[r]:at[r] + caps[r]]

    def product(k, j):
        s = k * parts + j
        weights(s + 1, start)
        weights(s, wait)

        def add(slot):
            for n in range(width // NB):
                b = pl.ds(pl.multiple_of(j * width + n * NB, NB), NB)
                for r in range(E):
                    rows = slice(N * at[r], N * (at[r] + caps[r]))
                    for half, acc in ((0, acc_g), (1, acc_u)):
                        w = buffer(slot)[perm[r], half, :, n * NB:(n + 1) * NB]
                        acc[rows, b] = acc[rows, b] + dot(z[rows], w)

        in_slot(lax.rem(s, 2), add)

    def middle(k):
        @pl.when(k + 5 < NK)
        def _():
            way.own(k + 5, start)

        @pl.when(k + 1 == EARLY)
        def _():
            way.crossed(EARLY)

        @pl.when(jnp.logical_and(k + 1 > EARLY, k + 1 < NK))
        def _():
            way.complete(k + 1)

        pl.when(k + 1 >= EARLY)(lambda: tokens(k + 1, start))

    def end(k):
        @pl.when(k + 3 < NK)
        def _():
            way.forward(k + 3)

        @pl.when(k + 2 < NK)
        def _():
            way.hand_over(k + 2)

    def chunk(k, c):
        gather(k)

        def part(j, c):
            product(k, j)
            pl.when(j == parts // 2 - 1)(lambda: middle(k))
            return c

        lax.fori_loop(0, parts, part, 0)
        end(k)
        return c

    lax.fori_loop(0, NK, chunk, 0)

    def store(n, r, run):
        rows = slice(N * at[r], N * (at[r] + caps[r]))
        run(pltpu.make_async_copy(z.at[rows], h.at[rows, pl.ds(pl.multiple_of(n * KB, KB), KB)], z_sem.at[r]))

    def finish(n, c):
        lanes = pl.ds(pl.multiple_of(n * KB, KB), KB)
        for r in range(E):
            rows = slice(N * at[r], N * (at[r] + caps[r]))

            @pl.when(n > 0)
            def _():
                store(n - 1, r, wait)

            z[rows] = (jax.nn.silu(acc_g[rows, lanes]) * acc_u[rows, lanes]).astype(BF16)
            store(n, r, start)
        return c

    lax.fori_loop(0, FF // KB, finish, 0)
    for r in range(E):
        store(FF // KB - 1, r, wait)

    def drain(k, c):
        pl.when(k > EARLY)(lambda: way.own(k, wait_send))
        way.drain(k)
        return c

    lax.fori_loop(EARLY, NK, drain, 0)


def down_kernel(
    caps, plan, h, tables, wd, sh, sd, y,
    hv, w0, w1, sv, shv, tv, comb, out, d_out, d_in, p_out, p_in, q_out, q_in, part, own, yv,
    h_sem, w_sem, s_sem, m_sem, y_sem, d_send, d_recv, p_send, p_recv, q_send, q_recv,
):
    seg, at = sum(caps), bases(caps)
    me = lax.axis_index("ep")
    cn, xn, yn, dg = around(me)
    perm = ranks(caps, plan)

    def lanes(n):
        return pl.ds(pl.multiple_of(n * CB, CB), CB)

    buffer, in_slot = buffers(caps, w0, w1)

    def weights(n, run):
        def copies(slot):
            for e in range(E):
                run(pltpu.make_async_copy(wd.at[e, :, lanes(n)], buffer(slot).at[e], w_sem.at[slot, e]))

        in_slot(n % 2, copies)

    def shared(n, run):
        slot = lax.rem(n, 2)
        run(pltpu.make_async_copy(sd.at[:, lanes(n)], sv.at[slot], s_sem.at[slot]))

    def activations(r, run):
        rows = slice(N * at[r], N * (at[r] + caps[r]))
        run(pltpu.make_async_copy(h.at[rows], hv.at[rows], h_sem.at[r]))

    load_tables = pltpu.make_async_copy(tables, tv, m_sem.at[0])
    load_tables.start()
    weights(0, start)
    for r in range(E):
        activations(r, start)
    load_sh = pltpu.make_async_copy(sh, shv, m_sem.at[1])
    load_sh.start()
    shared(0, start)
    greet((cn, xn, yn))

    def product(slot, r):
        v = dot(hv[N * at[r]:N * (at[r] + caps[r])], buffer(slot)[perm[r]]).astype(BF16)
        for b in range(N):
            out[slot, b, at[r]:at[r] + caps[r]] = v[b * caps[r]:(b + 1) * caps[r]]

    def combines():
        load_tables.wait()
        wide = comb.shape[-1]

        def one(b, c):
            v = []
            for r in range(E):
                key = (lax.broadcasted_iota(jnp.int32, (caps[r], T), 0) + (me * E + perm[r]) * CAP).astype(F32)
                w = jnp.zeros((caps[r], T), F32)
                for j in range(TOP):
                    w = jnp.where(tv[b, j:j + 1, :] == key, tv[b, TOP + j:TOP + j + 1, :], w)
                v.append(w)
            v.append(jnp.zeros((wide - seg, T), F32))
            comb[b] = jnp.concatenate(v).T.astype(BF16)
            return c

        lax.fori_loop(0, N, one, 0)

    combines()

    def summed(b, n):
        return dot(comb[b][:, :seg], out[lax.rem(n, 2), b])

    left, right = slice(0, HB), slice(HB, CB)

    def to_partner(n, run):
        slot = lax.rem(n, 2)
        run(remote(d_out.at[slot], d_in.at[slot], d_send.at[slot], d_recv.at[n], cn))

    def first_hop(n, run):
        slot = lax.rem(n, 2)
        for i, d in enumerate((xn, yn)):
            run(remote(p_out.at[slot, i], p_in.at[lax.rem(n, 6), i], p_send.at[slot, i], p_recv.at[n, i], d))

    def second_hop(n, run):
        slot = lax.rem(n, 2)
        for i, d in enumerate((yn, xn)):
            run(remote(q_out.at[slot, i], q_in.at[lax.rem(n, 4), i], q_send.at[slot, i], q_recv.at[n, i], d))

    def result(n, run):
        slot = lax.rem(n, 2)
        run(pltpu.make_async_copy(yv.at[slot], y.at[:, lanes(n)], y_sem.at[slot]))

    def for_partner(n, slot):
        for i, b in enumerate((cn,) + around(cn)[1:]):
            d_out[slot, i] = dot(comb[b][:, :seg], out[slot, b]).astype(BF16)

    def for_first(n):
        slot = lax.rem(n, 2)
        v = [summed(b, n) + d_in[slot, i].astype(F32) for i, b in ((3, dg), (1, xn), (2, yn), (0, me))]
        p_out[slot, 0, 1] = v[0][:, left].astype(BF16)
        p_out[slot, 1, 1] = v[0][:, right].astype(BF16)
        p_out[slot, 0, 0] = v[1][:, left].astype(BF16)
        part[lax.rem(n, 3), 1] = v[1][:, right]
        p_out[slot, 1, 0] = v[2][:, right].astype(BF16)
        part[lax.rem(n, 3), 0] = v[2][:, left]
        own[lax.rem(n, 5)] = v[3]

    def for_second(n):
        for i in range(2):
            q_out[lax.rem(n, 2), i] = (part[lax.rem(n, 3), i] + p_in[lax.rem(n, 6), i, 1].astype(F32)).astype(BF16)

    def for_own(n):
        v = own[lax.rem(n, 5)] + dot(shv[...], sv[lax.rem(n, 2)])
        for i, half in enumerate((left, right)):
            w = v[:, half] + p_in[lax.rem(n, 6), i, 0].astype(F32) + q_in[lax.rem(n, 4), i].astype(F32)
            yv[lax.rem(n, 2), :, half] = w.astype(BF16)

    def ready_first(n):
        @pl.when(n >= 2)
        def _():
            first_hop(n - 2, wait_send)

        to_partner(n, wait_recv)

    def ready_second(n):
        @pl.when(n >= 2)
        def _():
            second_hop(n - 2, wait_send)

        first_hop(n, wait_recv)

    def ready_own(n):
        @pl.when(n >= 2)
        def _():
            result(n - 2, wait)

        shared(n, wait)
        second_hop(n, wait_recv)

    stages = (
        (1, ready_first, for_first, first_hop),
        (3, ready_second, for_second, second_hop),
        (5, ready_own, for_own, result),
    )

    def step(i, c):
        @pl.when(i + 1 < NC)
        def _():
            weights(i + 1, start)

        @pl.when(jnp.logical_and(i >= 5, i - 4 < NC))
        def _():
            shared(i - 4, start)

        @pl.when(i == 0)
        def _():
            load_sh.wait()
            for r in range(E):
                activations(r, wait)

        @pl.when(i < NC)
        def _():
            weights(i, wait)

            def half(slot):
                for r in range(E // 2):
                    product(slot, r)

            in_slot(lax.rem(i, 2), half)

        inner = jnp.logical_and(i >= 5, i <= NC)

        @pl.when(inner)
        def _():
            for lag, ready, _, _ in stages:
                ready(i - lag)
            for lag, _, compute, _ in stages:
                compute(i - lag)
            for lag, _, _, go in stages:
                go(i - lag, start)

        @pl.when(jnp.logical_not(inner))
        def _():
            for lag, ready, compute, go in stages:
                n = i - lag

                @pl.when(jnp.logical_and(n >= 0, n < NC))
                def _():
                    ready(n)
                    compute(n)
                    go(n, start)

        @pl.when(i < NC)
        def _():
            @pl.when(i >= 2)
            def _():
                to_partner(i - 2, wait_send)

            def half(slot):
                for r in range(E // 2, E):
                    product(slot, r)
                for_partner(i, slot)

            in_slot(lax.rem(i, 2), half)
            to_partner(i, start)

        return c

    lax.fori_loop(0, NC + 5, step, 0)
    for n in (NC - 2, NC - 1):
        to_partner(n, wait_send)
        first_hop(n, wait_send)
        second_hop(n, wait_send)
        result(n, wait)


ANY = pl.BlockSpec(memory_space=pl.ANY)
SMEM = pl.BlockSpec(memory_space=pltpu.SMEM)
DMA = pltpu.SemaphoreType.DMA


def params(i):
    return pltpu.CompilerParams(collective_id=i, has_side_effects=True, vmem_limit_bytes=VMEM_LIMIT)


def share(expert, slot, gate, x, sg, su):
    return pl.pallas_call(
        share_kernel,
        name="share",
        out_shape=(
            jax.ShapeDtypeStruct((N, T, D), BF16),
            jax.ShapeDtypeStruct((N, ROWS, T), F32),
            jax.ShapeDtypeStruct((N, E, CAP, T), BF16),
            jax.ShapeDtypeStruct((TOP, 128), jnp.int32),
            jax.ShapeDtypeStruct((1,), jnp.int32),
            jax.ShapeDtypeStruct((T, FF), BF16),
        ),
        in_specs=[pl.BlockSpec(memory_space=pltpu.VMEM)] * 3 + [ANY] * 3,
        out_specs=(ANY,) * 4 + (SMEM, ANY),
        scratch_shapes=[
            pltpu.VMEM((ROWS, T), F32),
            pltpu.VMEM((N, ROWS, T), F32),
            pltpu.VMEM((TOP, 128), jnp.int32),
            pltpu.VMEM((N, E, CAP, T), BF16),
            pltpu.VMEM((NK, T, KB), BF16),
            pltpu.VMEM((SRING, 2, KB, FF), BF16),
            pltpu.VMEM((T, FF), F32),
            pltpu.VMEM((T, FF), F32),
            pltpu.VMEM((T, FF), BF16),
            DMA((NK,)),
            DMA((SRING, 2)),
            DMA((4,)),
            DMA((N - 1,)),
            DMA((N - 1,)),
        ]
        + way_semaphores(EARLY + 1),
        compiler_params=params(0),
    )(expert, slot, gate, x, sg, su)


def up(caps, width, identity, plan, x, xg, picks, wg, wu):
    seg = sum(caps)
    return pl.pallas_call(
        functools.partial(up_kernel, caps),
        name="up",
        out_shape=(jax.ShapeDtypeStruct((N, T, D), BF16), jax.ShapeDtypeStruct((N * seg, FF), BF16)),
        input_output_aliases={2: 0},
        in_specs=[SMEM] + [ANY] * 5,
        out_specs=(ANY,) * 2,
        scratch_shapes=[
            pltpu.VMEM((N * seg, FF), F32),
            pltpu.VMEM((N * seg, FF), F32),
            pltpu.VMEM((N * seg, KB), BF16),
            pltpu.VMEM((2, N, T, KB), BF16),
            pltpu.VMEM((2, E, 2, KB, width) if caps == FULL else (E, 2, KB, width), BF16),
            pltpu.VMEM((16, 128) if caps == FULL else (E, 2, KB, width), BF16),
            pltpu.VMEM((N, E, CAP, T), BF16),
            DMA((2, E, 2)),
            DMA((2, N)),
            DMA((E,)),
            DMA,
        ]
        + way_semaphores(NK),
        compiler_params=params(identity),
    )(plan, x, xg, picks, wg, wu)[1]


def down(caps, identity, plan, h, tables, wd, sh, sd):
    seg = sum(caps)
    return pl.pallas_call(
        functools.partial(down_kernel, caps),
        name="down",
        out_shape=jax.ShapeDtypeStruct((T, D), BF16),
        in_specs=[SMEM] + [ANY] * 5,
        out_specs=ANY,
        scratch_shapes=[
            pltpu.VMEM((N * seg, FF), BF16),
            pltpu.VMEM((2, E, FF, CB) if caps == FULL else (E, FF, CB), BF16),
            pltpu.VMEM((16, 128) if caps == FULL else (E, FF, CB), BF16),
            pltpu.VMEM((2, FF, CB), BF16),
            pltpu.VMEM((T, FF), BF16),
            pltpu.VMEM((N, ROWS, T), F32),
            pltpu.VMEM((N, T, -(-seg // 128) * 128), BF16),
            pltpu.VMEM((2, N, seg, CB), BF16),
            pltpu.VMEM((2, 4, T, CB), BF16),
            pltpu.VMEM((2, 4, T, CB), BF16),
            pltpu.VMEM((2, 2, 2, T, HB), BF16),
            pltpu.VMEM((6, 2, 2, T, HB), BF16),
            pltpu.VMEM((2, 2, T, HB), BF16),
            pltpu.VMEM((4, 2, T, HB), BF16),
            pltpu.VMEM((3, 2, T, HB), F32),
            pltpu.VMEM((5, T, CB), F32),
            pltpu.VMEM((2, T, CB), BF16),
            DMA((E,)),
            DMA((2, E)),
            DMA((2,)),
            DMA((2,)),
            DMA((2,)),
            DMA((2,)),
            DMA((NC,)),
            DMA((2, 2)),
            DMA((NC, 2)),
            DMA((2, 2)),
            DMA((NC, 2)),
        ],
        compiler_params=params(identity),
    )(plan, h, tables, wd, sh, sd)


def solution(mesh):
    def device(x, expert, slot, gate, wg, wu, wd, sg, su, sd):
        x, expert, slot, gate = x[0, 0], expert[0, 0], slot[0, 0], gate[0, 0]
        xg, tables, picks, plan, wide, sh = share(expert.T, slot.T, gate.T, x, sg, su)

        def experts(caps, width, identity):
            h = up(caps, width, identity, plan, x, xg, picks, wg, wu)
            return down(caps, identity + 1, plan, h, tables, wd, sh, sd)

        y = lax.switch(wide[0], (lambda: experts(NARROW, 1024, 1), lambda: experts(FULL, 512, 3)))
        return y[None, None]

    tokens, experts = P("dp", "ep"), P("ep")
    return jax.shard_map(
        device,
        mesh=mesh,
        in_specs=(tokens,) * 4 + (experts,) * 3 + (P(),) * 3,
        out_specs=tokens,
        check_vma=False,
    )
```

```python
import functools

import jax
import jax.numpy as jnp
from jax import lax
from jax.experimental import pallas as pl
from jax.experimental.pallas import tpu as pltpu
from jax.sharding import PartitionSpec as P

MESH = pl.DeviceIdType.MESH
F32, BF16 = jnp.float32, jnp.bfloat16
N = 8
T = 256
D = 7168
FF = 2048
TOP = 8
E = 4
EXPERTS = N * E
CAP = 80
SEG = E * CAP
KB = 512
NK = D // KB
EARLY = 2
NB = 512
CB = 512
HB = CB // 2
NC = D // CB
SRING = 4
ROWS = 3 * TOP
FULL = (CAP,) * E
NARROW = (80, 80, 80, 32)
VMEM_LIMIT = 67043328

start, wait = (lambda c: c.start()), (lambda c: c.wait())
wait_send, wait_recv = (lambda c: c.wait_send()), (lambda c: c.wait_recv())


def around(me):
    i, j, c = me // 4, (me // 2) % 2, me % 2
    at = lambda i, j, c: i * 4 + j * 2 + c
    return at(i, j, 1 - c), at(1 - i, j, c), at(i, 1 - j, c), at(1 - i, 1 - j, c)


def greet(devices):
    barrier = pltpu.get_barrier_semaphore()
    for d in devices:
        pl.semaphore_signal(barrier, inc=1, device_id={"ep": d}, device_id_type=MESH)
    pl.semaphore_wait(barrier, len(devices))


def remote(src, dst, send, recv, to):
    return pltpu.make_async_remote_copy(
        src_ref=src, dst_ref=dst, send_sem=send, recv_sem=recv, device_id={"ep": to}, device_id_type=MESH
    )


def dot(a, b):
    return jnp.dot(a, b, preferred_element_type=F32)


def cols(k):
    return pl.ds(pl.multiple_of(k * KB, KB), KB)


class Way:
    def __init__(self, x, xg, sems):
        self.x, self.xg = x, xg
        self.o_send, self.o_recv, self.f_send, self.f_recv, self.c_send, self.c_recv = sems
        self.me = lax.axis_index("ep")
        self.cn, self.xn, self.yn, self.dg = around(self.me)

    def part(self, b, k):
        return self.xg.at[b, :, cols(k)]

    def own(self, k, run):
        for i, d in enumerate((self.xn, self.yn, self.cn)):
            run(remote(self.x.at[:, cols(k)], self.part(self.me, k), self.o_send.at[i, k], self.o_recv.at[i, k], d))

    def half(self, b, k, i):
        return self.xg.at[b, :, pl.ds(pl.multiple_of(k * KB + i * (KB // 2), KB // 2), KB // 2)]

    def onward(self, k, run):
        for i, (src, to) in enumerate(((self.xn, self.yn), (self.yn, self.xn))):
            part = self.half(src, k, i)
            run(remote(part, part, self.f_send.at[i, k], self.f_recv.at[i, k], to))

    def across(self, i, src, k, run):
        part = self.part(src, k)
        run(remote(part, part, self.c_send.at[i, k], self.c_recv.at[i, k], self.cn))

    def arrived(self, i, src, k):
        part = self.part(src, k)
        remote(part, part, self.o_send.at[i, k], self.o_recv.at[i, k], src).wait_recv()

    def forward(self, k):
        self.arrived(0, self.xn, k)
        self.arrived(1, self.yn, k)
        self.pass_on(k)

    def pass_on(self, k):
        self.onward(k, start)
        self.across(0, self.xn, k, start)
        self.across(1, self.yn, k, start)

    def landed(self, k):
        for i, src in enumerate((self.yn, self.xn)):
            part = self.half(self.dg, k, i)
            remote(part, part, self.f_send.at[i, k], self.f_recv.at[i, k], src).wait_recv()

    def hand_over(self, k):
        self.landed(k)
        self.across(2, self.dg, k, start)

    def complete(self, k):
        self.arrived(2, self.cn, k)
        self.crossed(k)

    def crossed(self, k):
        for i in range(3):
            part = self.part(self.cn, k)
            remote(part, part, self.c_send.at[i, k], self.c_recv.at[i, k], self.cn).wait_recv()

    def drain(self, k):
        self.onward(k, wait_send)
        for i, src in enumerate((self.xn, self.yn, self.dg)):
            self.across(i, src, k, wait_send)


def way_semaphores(chunks):
    dma = pltpu.SemaphoreType.DMA
    return [dma((3, chunks)), dma((3, chunks)), dma((2, chunks)), dma((2, chunks)), dma((3, chunks)), dma((3, chunks))]


def share_kernel(
    expert, slot, gate, x, sg, su, xg, tables, picks, plan, wide, sh,
    mine, tv, pv, pick, xv, wv, acc_g, acc_u, hv, x_sem, w_sem, h_sem, t_send, t_recv, *sems,
):
    me = lax.axis_index("ep")
    others = [lax.rem(me + d, N) for d in range(1, N)]
    way = Way(x, xg, sems)

    def weights(s, run):
        at = lax.rem(s, SRING)
        for half, ref in ((0, sg), (1, su)):
            run(pltpu.make_async_copy(ref.at[cols(s)], wv.at[at, half], w_sem.at[at, half]))

    def tokens(s, run):
        run(pltpu.make_async_copy(x.at[:, cols(s)], xv.at[s], x_sem.at[s]))

    for s in range(SRING - 1):
        tokens(s, start)
        weights(s, start)

    key = jnp.where(slot[...] < CAP, expert[...] * CAP + slot[...], -1).astype(F32)
    mine[:TOP] = key
    mine[TOP:2 * TOP] = gate[...].astype(BF16).astype(F32)
    key = jnp.concatenate([key, jnp.zeros((128 - TOP, T), F32)]).T
    low = (lax.broadcasted_iota(jnp.int32, (T, 128), 1) * CAP).astype(F32)
    used = jnp.zeros((T, 128), F32)
    for j in range(TOP):
        depth = key[:, j:j + 1] - low
        used = jnp.maximum(used, jnp.where((depth >= 0) & (depth < CAP), depth + 1, 0.0))
    used = jnp.max(used, axis=0, keepdims=True)
    mine[2 * TOP:] = jnp.broadcast_to(jnp.concatenate([used, used], axis=1), (TOP, T))

    greet(others)
    for i, d in enumerate(others):
        remote(mine, tv.at[me], t_send.at[i], t_recv.at[N - 2 - i], d).start()
    for k in range(EARLY):
        way.own(k, start)
    for s in range(SRING - 1, NK):
        tokens(s, start)
    tv[me] = mine[...]

    def project(s):
        for n in range(FF // NB):
            b = slice(n * NB, (n + 1) * NB)
            for half, acc in ((0, acc_g), (1, acc_u)):
                acc[:, b] = acc[:, b] + dot(xv[s], wv[lax.rem(s, SRING), half, :, b])

    def ready(s):
        @pl.when(s + SRING - 1 < NK)
        def _():
            weights(s + SRING - 1, start)

        tokens(s, wait)
        weights(s, wait)

    acc_g[...] = jnp.zeros((T, FF), F32)
    acc_u[...] = jnp.zeros((T, FF), F32)

    def first_steps(s, c):
        ready(s)
        project(s)
        return c

    lax.fori_loop(0, NK - N - 1, first_steps, 0)
    for i, b in enumerate(others):
        remote(mine, tv.at[b], t_send.at[i], t_recv.at[i], b).wait_recv()
    keep = pltpu.make_async_copy(tv, tables, h_sem.at[0])
    keep.start()

    row = (lax.broadcasted_iota(jnp.int32, (SEG, T), 0) + me * SEG).astype(F32)

    def last_steps(s, c):
        ready(s)
        b = jnp.minimum(s - (NK - N - 1), N - 1)
        hit = tv[b, :1, :] == row
        for j in range(1, TOP):
            hit = hit | (tv[b, j:j + 1, :] == row)
        hit = jnp.where(hit, 1.0, 0.0).astype(BF16)
        for e in range(E):
            pick[b, e] = hit[e * CAP:(e + 1) * CAP]
        project(s)

        @pl.when(s == 6)
        def _():
            way.forward(0)

        @pl.when(s == 9)
        def _():
            way.forward(1)
            way.own(2, start)

        @pl.when(s == 12)
        def _():
            way.hand_over(0)

        return c

    lax.fori_loop(NK - N - 1, NK, last_steps, 0)
    keep_picks = pltpu.make_async_copy(pick, picks, h_sem.at[3])
    keep_picks.start()
    way.hand_over(1)

    n = tv[0, 2 * TOP:, :128]
    for b in range(1, N):
        n = jnp.maximum(n, tv[b, 2 * TOP:, :128])
    lane = lax.broadcasted_iota(jnp.int32, n.shape, 1)
    e = lane % E
    rank = jnp.zeros(n.shape, jnp.int32)
    for o in range(1, E):
        later = e + o < E
        other = jnp.where(later, pltpu.roll(n, 128 - o, 1), pltpu.roll(n, E - o, 1))
        rank = rank + ((other > n) | ((other == n) & jnp.logical_not(later))).astype(jnp.int32)
    caps = jnp.zeros(n.shape, F32)
    for r in range(E):
        caps = jnp.where(rank == r, float(NARROW[r]), caps)
    wide[0] = jnp.max(jnp.where((n > caps) & (lane < EXPERTS), 1.0, 0.0)).astype(jnp.int32)
    out = jnp.zeros(n.shape, F32)
    for r in range(E):
        chosen = jnp.where((lane // E == me) & (rank == r), e, 0).astype(F32)
        out = out + jnp.where(lane == r, jnp.sum(chosen, axis=1, keepdims=True), 0.0)
    pv[...] = out.astype(jnp.int32)

    hv[...] = (jax.nn.silu(acc_g[...]) * acc_u[...]).astype(BF16)
    keep_plan = pltpu.make_async_copy(pv, plan, h_sem.at[2])
    keep_plan.start()
    keep_sh = pltpu.make_async_copy(hv, sh, h_sem.at[1])
    keep_sh.start()
    for i, d in enumerate(others):
        remote(mine, tv.at[me], t_send.at[i], t_recv.at[N - 2 - i], d).wait_send()
    for k in range(EARLY):
        way.complete(k)
        way.own(k, wait_send)
        way.drain(k)
    for i, src in enumerate((way.xn, way.yn, way.cn)):
        way.arrived(i, src, EARLY)
    way.own(EARLY, wait_send)
    keep.wait()
    keep_plan.wait()
    keep_picks.wait()
    keep_sh.wait()


def buffers(caps, w0, w1):
    full = caps == FULL
    buffer = lambda slot: w0.at[slot] if full else (w0, w1)[slot]

    def in_slot(slot, f):
        if full or isinstance(slot, int):
            f(slot)
        else:
            for q in range(2):
                pl.when(slot == q)(functools.partial(f, q))

    return buffer, in_slot


def bases(caps):
    return [sum(caps[:r]) for r in range(E)]


def ranks(caps, plan):
    return list(range(E)) if caps == FULL else [plan[0, r] for r in range(E)]


def up_kernel(
    caps, plan, x, _, picks, wg, wu, xg, h, acc_g, acc_u, z, xv, w0, w1, pick, w_sem, x_sem, z_sem, p_sem, *sems
):
    seg, at = sum(caps), bases(caps)
    width = w0.shape[-1]
    parts = FF // width
    me = lax.axis_index("ep")
    way = Way(x, xg, sems)
    perm = ranks(caps, plan)
    buffer, in_slot = buffers(caps, w0, w1)

    def weights(s, run):
        def copies(slot):
            k, lanes = s // parts, pl.ds(pl.multiple_of(lax.rem(s, parts) * width, width), width)
            for e in range(E):
                for half, ref in ((0, wg), (1, wu)):
                    run(pltpu.make_async_copy(ref.at[e, cols(k), lanes], buffer(slot).at[e, half], w_sem.at[slot, e, half]))

        pl.when(s < NK * parts)(lambda: in_slot(lax.rem(s, 2), copies))

    def tokens(k, run):
        slot = lax.rem(k, 2)

        @pl.when(k < NK)
        def _():
            for d in range(1, N):
                b = lax.rem(me + d, N)
                run(pltpu.make_async_copy(way.part(b, k), xv.at[slot, b], x_sem.at[slot, b]))
            run(pltpu.make_async_copy(x.at[:, cols(k)], xv.at[slot, me], x_sem.at[slot, me]))

    load_picks = pltpu.make_async_copy(picks, pick, p_sem)
    load_picks.start()
    tokens(0, start)
    weights(0, start)
    greet((way.cn, way.xn, way.yn))
    way.pass_on(EARLY)
    way.own(EARLY + 1, start)
    way.own(EARLY + 2, start)

    def clear(i, c):
        rows = pl.ds(pl.multiple_of(i * 64, 64), 64)
        acc_g[rows] = jnp.zeros((64, FF), F32)
        acc_u[rows] = jnp.zeros((64, FF), F32)
        return c

    lax.fori_loop(0, N * seg // 64, clear, 0)
    load_picks.wait()
    tokens(1, start)

    def gather(k):
        slot = lax.rem(k, 2)
        tokens(k, wait)
        for b in range(N):
            hit = jnp.concatenate([pick[b, perm[r]][:caps[r]] for r in range(E)])
            v = dot(hit, xv[slot, b]).astype(BF16)
            for r in range(E):
                z[N * at[r] + b * caps[r]:N * at[r] + (b + 1) * caps[r]] = v[at[r]:at[r] + caps[r]]

    def product(k, j):
        s = k * parts + j
        weights(s + 1, start)
        weights(s, wait)

        def add(slot):
            for n in range(width // NB):
                b = pl.ds(pl.multiple_of(j * width + n * NB, NB), NB)
                for r in range(E):
                    rows = slice(N * at[r], N * (at[r] + caps[r]))
                    for half, acc in ((0, acc_g), (1, acc_u)):
                        w = buffer(slot)[perm[r], half, :, n * NB:(n + 1) * NB]
                        acc[rows, b] = acc[rows, b] + dot(z[rows], w)

        in_slot(lax.rem(s, 2), add)

    def middle(k):
        @pl.when(k + 5 < NK)
        def _():
            way.own(k + 5, start)

        @pl.when(k + 1 == EARLY)
        def _():
            way.crossed(EARLY)

        @pl.when(jnp.logical_and(k + 1 > EARLY, k + 1 < NK))
        def _():
            way.complete(k + 1)

        pl.when(k + 1 >= EARLY)(lambda: tokens(k + 1, start))

    def end(k):
        @pl.when(k + 3 < NK)
        def _():
            way.forward(k + 3)

        @pl.when(k + 2 < NK)
        def _():
            way.hand_over(k + 2)

    def chunk(k, c):
        gather(k)

        def part(j, c):
            product(k, j)
            pl.when(j == parts // 2 - 1)(lambda: middle(k))
            return c

        lax.fori_loop(0, parts, part, 0)
        end(k)
        return c

    lax.fori_loop(0, NK, chunk, 0)

    def store(n, r, run):
        rows = slice(N * at[r], N * (at[r] + caps[r]))
        run(pltpu.make_async_copy(z.at[rows], h.at[rows, pl.ds(pl.multiple_of(n * KB, KB), KB)], z_sem.at[r]))

    def finish(n, c):
        lanes = pl.ds(pl.multiple_of(n * KB, KB), KB)
        for r in range(E):
            rows = slice(N * at[r], N * (at[r] + caps[r]))

            @pl.when(n > 0)
            def _():
                store(n - 1, r, wait)

            z[rows] = (jax.nn.silu(acc_g[rows, lanes]) * acc_u[rows, lanes]).astype(BF16)
            store(n, r, start)
        return c

    lax.fori_loop(0, FF // KB, finish, 0)
    for r in range(E):
        store(FF // KB - 1, r, wait)

    def drain(k, c):
        pl.when(k > EARLY)(lambda: way.own(k, wait_send))
        way.drain(k)
        return c

    lax.fori_loop(EARLY, NK, drain, 0)


def down_kernel(
    caps, plan, h, tables, wd, sh, sd, y,
    hv, w0, w1, sv, shv, tv, comb, out, d_out, d_in, p_out, p_in, q_out, q_in, part, own, yv,
    h_sem, w_sem, s_sem, m_sem, y_sem, d_send, d_recv, p_send, p_recv, q_send, q_recv,
):
    seg, at = sum(caps), bases(caps)
    me = lax.axis_index("ep")
    cn, xn, yn, dg = around(me)
    perm = ranks(caps, plan)

    def lanes(n):
        return pl.ds(pl.multiple_of(n * CB, CB), CB)

    buffer, in_slot = buffers(caps, w0, w1)

    def weights(n, run):
        def copies(slot):
            for e in range(E):
                run(pltpu.make_async_copy(wd.at[e, :, lanes(n)], buffer(slot).at[e], w_sem.at[slot, e]))

        in_slot(n % 2, copies)

    def shared(n, run):
        slot = lax.rem(n, 2)
        run(pltpu.make_async_copy(sd.at[:, lanes(n)], sv.at[slot], s_sem.at[slot]))

    def activations(r, run):
        rows = slice(N * at[r], N * (at[r] + caps[r]))
        run(pltpu.make_async_copy(h.at[rows], hv.at[rows], h_sem.at[r]))

    load_tables = pltpu.make_async_copy(tables, tv, m_sem.at[0])
    load_tables.start()
    weights(0, start)
    for r in range(E):
        activations(r, start)
    load_sh = pltpu.make_async_copy(sh, shv, m_sem.at[1])
    greet((cn, xn, yn))

    def product(slot, r):
        v = dot(hv[N * at[r]:N * (at[r] + caps[r])], buffer(slot)[perm[r]]).astype(BF16)
        for b in range(N):
            out[slot, b, at[r]:at[r] + caps[r]] = v[b * caps[r]:(b + 1) * caps[r]]

    def combines():
        load_tables.wait()
        wide = comb.shape[-1]

        def one(b, c):
            v = []
            for r in range(E):
                key = (lax.broadcasted_iota(jnp.int32, (caps[r], T), 0) + (me * E + perm[r]) * CAP).astype(F32)
                w = jnp.zeros((caps[r], T), F32)
                for j in range(TOP):
                    w = jnp.where(tv[b, j:j + 1, :] == key, tv[b, TOP + j:TOP + j + 1, :], w)
                v.append(w)
            v.append(jnp.zeros((wide - seg, T), F32))
            comb[b] = jnp.concatenate(v).T.astype(BF16)
            return c

        lax.fori_loop(0, N, one, 0)

    combines()

    def summed(b, n):
        return dot(comb[b][:, :seg], out[lax.rem(n, 2), b])

    left, right = slice(0, HB), slice(HB, CB)

    def to_partner(n, run):
        slot = lax.rem(n, 2)
        run(remote(d_out.at[slot], d_in.at[slot], d_send.at[slot], d_recv.at[n], cn))

    def first_hop(n, run):
        slot = lax.rem(n, 2)
        for i, d in enumerate((xn, yn)):
            run(remote(p_out.at[slot, i], p_in.at[lax.rem(n, 6), i], p_send.at[slot, i], p_recv.at[n, i], d))

    def second_hop(n, run):
        slot = lax.rem(n, 2)
        for i, d in enumerate((yn, xn)):
            run(remote(q_out.at[slot, i], q_in.at[lax.rem(n, 4), i], q_send.at[slot, i], q_recv.at[n, i], d))

    def result(n, run):
        slot = lax.rem(n, 2)
        run(pltpu.make_async_copy(yv.at[slot], y.at[:, lanes(n)], y_sem.at[slot]))

    def for_partner(n, slot):
        for i, b in enumerate((cn,) + around(cn)[1:]):
            d_out[slot, i] = dot(comb[b][:, :seg], out[slot, b]).astype(BF16)

    def for_first(n):
        slot = lax.rem(n, 2)
        v = [summed(b, n) + d_in[slot, i].astype(F32) for i, b in ((3, dg), (1, xn), (2, yn), (0, me))]
        p_out[slot, 0, 1] = v[0][:, left].astype(BF16)
        p_out[slot, 1, 1] = v[0][:, right].astype(BF16)
        p_out[slot, 0, 0] = v[1][:, left].astype(BF16)
        part[lax.rem(n, 3), 1] = v[1][:, right]
        p_out[slot, 1, 0] = v[2][:, right].astype(BF16)
        part[lax.rem(n, 3), 0] = v[2][:, left]
        own[lax.rem(n, 5)] = v[3]

    def for_second(n):
        for i in range(2):
            q_out[lax.rem(n, 2), i] = (part[lax.rem(n, 3), i] + p_in[lax.rem(n, 6), i, 1].astype(F32)).astype(BF16)

    def for_own(n):
        v = own[lax.rem(n, 5)] + dot(shv[...], sv[lax.rem(n, 2)])
        for i, half in enumerate((left, right)):
            w = v[:, half] + p_in[lax.rem(n, 6), i, 0].astype(F32) + q_in[lax.rem(n, 4), i].astype(F32)
            yv[lax.rem(n, 2), :, half] = w.astype(BF16)

    def ready_first(n):
        @pl.when(n >= 2)
        def _():
            first_hop(n - 2, wait_send)

        to_partner(n, wait_recv)

    def ready_second(n):
        @pl.when(n >= 2)
        def _():
            second_hop(n - 2, wait_send)

        first_hop(n, wait_recv)

    def ready_own(n):
        @pl.when(n >= 2)
        def _():
            result(n - 2, wait)

        shared(n, wait)
        second_hop(n, wait_recv)

    stages = (
        (1, ready_first, for_first, first_hop),
        (3, ready_second, for_second, second_hop),
        (5, ready_own, for_own, result),
    )

    def step(i, c):
        @pl.when(i + 1 < NC)
        def _():
            weights(i + 1, start)

        @pl.when(jnp.logical_and(i >= 5, i - 4 < NC))
        def _():
            shared(i - 4, start)

        @pl.when(i == 0)
        def _():
            for r in range(E):
                activations(r, wait)

        @pl.when(i == 2)
        def _():
            load_sh.start()
            shared(0, start)

        @pl.when(i == 4)
        def _():
            load_sh.wait()

        @pl.when(i < NC)
        def _():
            weights(i, wait)

            def half(slot):
                for r in range(E // 2):
                    product(slot, r)

            in_slot(lax.rem(i, 2), half)

        inner = jnp.logical_and(i >= 5, i <= NC)

        @pl.when(inner)
        def _():
            for lag, ready, _, _ in stages:
                ready(i - lag)
            for lag, _, compute, _ in stages:
                compute(i - lag)
            for lag, _, _, go in stages:
                go(i - lag, start)

        @pl.when(jnp.logical_not(inner))
        def _():
            for lag, ready, compute, go in stages:
                n = i - lag

                @pl.when(jnp.logical_and(n >= 0, n < NC))
                def _():
                    ready(n)
                    compute(n)
                    go(n, start)

        @pl.when(i < NC)
        def _():
            @pl.when(i >= 2)
            def _():
                to_partner(i - 2, wait_send)

            def half(slot):
                for r in range(E // 2, E):
                    product(slot, r)
                for_partner(i, slot)

            in_slot(lax.rem(i, 2), half)
            to_partner(i, start)

        return c

    lax.fori_loop(0, NC + 5, step, 0)
    for n in (NC - 2, NC - 1):
        to_partner(n, wait_send)
        first_hop(n, wait_send)
        second_hop(n, wait_send)
        result(n, wait)


ANY = pl.BlockSpec(memory_space=pl.ANY)
SMEM = pl.BlockSpec(memory_space=pltpu.SMEM)
DMA = pltpu.SemaphoreType.DMA


def params(i):
    return pltpu.CompilerParams(collective_id=i, has_side_effects=True, vmem_limit_bytes=VMEM_LIMIT)


def share(expert, slot, gate, x, sg, su):
    return pl.pallas_call(
        share_kernel,
        name="share",
        out_shape=(
            jax.ShapeDtypeStruct((N, T, D), BF16),
            jax.ShapeDtypeStruct((N, ROWS, T), F32),
            jax.ShapeDtypeStruct((N, E, CAP, T), BF16),
            jax.ShapeDtypeStruct((TOP, 128), jnp.int32),
            jax.ShapeDtypeStruct((1,), jnp.int32),
            jax.ShapeDtypeStruct((T, FF), BF16),
        ),
        in_specs=[pl.BlockSpec(memory_space=pltpu.VMEM)] * 3 + [ANY] * 3,
        out_specs=(ANY,) * 4 + (SMEM, ANY),
        scratch_shapes=[
            pltpu.VMEM((ROWS, T), F32),
            pltpu.VMEM((N, ROWS, T), F32),
            pltpu.VMEM((TOP, 128), jnp.int32),
            pltpu.VMEM((N, E, CAP, T), BF16),
            pltpu.VMEM((NK, T, KB), BF16),
            pltpu.VMEM((SRING, 2, KB, FF), BF16),
            pltpu.VMEM((T, FF), F32),
            pltpu.VMEM((T, FF), F32),
            pltpu.VMEM((T, FF), BF16),
            DMA((NK,)),
            DMA((SRING, 2)),
            DMA((4,)),
            DMA((N - 1,)),
            DMA((N - 1,)),
        ]
        + way_semaphores(EARLY + 1),
        compiler_params=params(0),
    )(expert, slot, gate, x, sg, su)


def up(caps, width, identity, plan, x, xg, picks, wg, wu):
    seg = sum(caps)
    return pl.pallas_call(
        functools.partial(up_kernel, caps),
        name="up",
        out_shape=(jax.ShapeDtypeStruct((N, T, D), BF16), jax.ShapeDtypeStruct((N * seg, FF), BF16)),
        input_output_aliases={2: 0},
        in_specs=[SMEM] + [ANY] * 5,
        out_specs=(ANY,) * 2,
        scratch_shapes=[
            pltpu.VMEM((N * seg, FF), F32),
            pltpu.VMEM((N * seg, FF), F32),
            pltpu.VMEM((N * seg, KB), BF16),
            pltpu.VMEM((2, N, T, KB), BF16),
            pltpu.VMEM((2, E, 2, KB, width) if caps == FULL else (E, 2, KB, width), BF16),
            pltpu.VMEM((16, 128) if caps == FULL else (E, 2, KB, width), BF16),
            pltpu.VMEM((N, E, CAP, T), BF16),
            DMA((2, E, 2)),
            DMA((2, N)),
            DMA((E,)),
            DMA,
        ]
        + way_semaphores(NK),
        compiler_params=params(identity),
    )(plan, x, xg, picks, wg, wu)[1]


def down(caps, identity, plan, h, tables, wd, sh, sd):
    seg = sum(caps)
    return pl.pallas_call(
        functools.partial(down_kernel, caps),
        name="down",
        out_shape=jax.ShapeDtypeStruct((T, D), BF16),
        in_specs=[SMEM] + [ANY] * 5,
        out_specs=ANY,
        scratch_shapes=[
            pltpu.VMEM((N * seg, FF), BF16),
            pltpu.VMEM((2, E, FF, CB) if caps == FULL else (E, FF, CB), BF16),
            pltpu.VMEM((16, 128) if caps == FULL else (E, FF, CB), BF16),
            pltpu.VMEM((2, FF, CB), BF16),
            pltpu.VMEM((T, FF), BF16),
            pltpu.VMEM((N, ROWS, T), F32),
            pltpu.VMEM((N, T, -(-seg // 128) * 128), BF16),
            pltpu.VMEM((2, N, seg, CB), BF16),
            pltpu.VMEM((2, 4, T, CB), BF16),
            pltpu.VMEM((2, 4, T, CB), BF16),
            pltpu.VMEM((2, 2, 2, T, HB), BF16),
            pltpu.VMEM((6, 2, 2, T, HB), BF16),
            pltpu.VMEM((2, 2, T, HB), BF16),
            pltpu.VMEM((4, 2, T, HB), BF16),
            pltpu.VMEM((3, 2, T, HB), F32),
            pltpu.VMEM((5, T, CB), F32),
            pltpu.VMEM((2, T, CB), BF16),
            DMA((E,)),
            DMA((2, E)),
            DMA((2,)),
            DMA((2,)),
            DMA((2,)),
            DMA((2,)),
            DMA((NC,)),
            DMA((2, 2)),
            DMA((NC, 2)),
            DMA((2, 2)),
            DMA((NC, 2)),
        ],
        compiler_params=params(identity),
    )(plan, h, tables, wd, sh, sd)


def solution(mesh):
    def device(x, expert, slot, gate, wg, wu, wd, sg, su, sd):
        x, expert, slot, gate = x[0, 0], expert[0, 0], slot[0, 0], gate[0, 0]
        xg, tables, picks, plan, wide, sh = share(expert.T, slot.T, gate.T, x, sg, su)

        def experts(caps, width, identity):
            h = up(caps, width, identity, plan, x, xg, picks, wg, wu)
            return down(caps, identity + 1, plan, h, tables, wd, sh, sd)

        y = lax.switch(wide[0], (lambda: experts(NARROW, 1024, 1), lambda: experts(FULL, 512, 3)))
        return y[None, None]

    tokens, experts = P("dp", "ep"), P("ep")
    return jax.shard_map(
        device,
        mesh=mesh,
        in_specs=(tokens,) * 4 + (experts,) * 3 + (P(),) * 3,
        out_specs=tokens,
        check_vma=False,
    )
```
